32 devices in a mesh: dp: 2 (over x), ty: 4 (over z), tx: 4 (over y, core).
Axes of the slice: x: 2, y: 2, z: 4, core: 2. Of those that a mesh axis runs over, the one named last changes fastest.
Arguments:
- x_in: bfloat16 [8, 1024, 2048], P(('dp', 'ty'), None, 'tx'), parts along dimension 0
- w_q: bfloat16 [2048, 2048], P('tx', 'ty')
- w_k: bfloat16 [2048, 2048], P('tx', 'ty')
- w_v: bfloat16 [2048, 2048], P('tx', 'ty')
- w_o: bfloat16 [2048, 2048], P('ty', 'tx')
- w_gate: bfloat16 [2048, 8192], P('tx', 'ty')
- w_up: bfloat16 [2048, 8192], P('tx', 'ty')
- w_down: bfloat16 [8192, 2048], P('ty', 'tx')
Outputs:
- output: bfloat16 [8, 1024, 2048], P(('dp', 'ty'), None, 'tx'), parts along dimension 0
There are 2 independent parts. The reference program is written for one: setup_inputs(seed, part) draws one part's arguments, and reference() takes and returns one part's arrays. A program takes and returns all parts, laid end to end along the dimension named above; an argument that names none is the same for every part.
All inputs are finite; a program needn't handle non-finite values.
Results may differ from the reference program's by a relative error of at most 0.02.
Values are sent between devices in bfloat16 or wider.
A program may use at most 1 GiB of HBM per device.

```python
import jax
import jax.numpy as jnp
from jax import lax

NSEQ = 4
SEQ = 1024
D = 2048
FF = 8192
HEADS = 16

HEAD_DIM = D // HEADS
EPS = 1e-5
THETA = 10000.0


def setup_inputs(seed: int = 0, part: int = 0) -> dict:
    root_key = jax.random.key(seed)
    act_root, weight_root = jax.random.split(root_key)
    part_key = jax.random.fold_in(act_root, part)
    key_tok, key_scale, key_shift, key_slope, key_walk = jax.random.split(part_key, 5)
    tok_noise = jax.random.normal(key_tok, (NSEQ, SEQ, D), jnp.float32)
    tok_scale = jax.random.uniform(key_scale, (NSEQ, SEQ, 1), jnp.float32, 0.5, 2.0)
    tok_shift = 0.5 * jax.random.normal(key_shift, (NSEQ, SEQ, 1), jnp.float32)
    col_slope = jax.random.uniform(key_slope, (), jnp.float32, 1.0, 2.0)
    col_pos = jnp.arange(D, dtype=jnp.float32) / D - 0.5
    col_walk = jnp.cumsum(jax.random.normal(key_walk, (D,), jnp.float32)) * (1.5 * D ** -0.5)
    col_offset = 2.0 * col_slope * col_pos + col_walk
    x_in = (tok_scale * tok_noise + tok_shift + col_offset).astype(jnp.bfloat16)
    weight_keys = jax.random.split(weight_root, 7)

    def draw_weight(key_w, fan_in, fan_out, gain_mul):
        return (gain_mul * fan_in ** -0.5 * jax.random.normal(key_w, (fan_in, fan_out), jnp.float32)).astype(jnp.bfloat16)

    return {
        "x_in": x_in,
        "w_q": draw_weight(weight_keys[0], D, D, 1.5),
        "w_k": draw_weight(weight_keys[1], D, D, 1.5),
        "w_v": draw_weight(weight_keys[2], D, D, 1.0),
        "w_o": draw_weight(weight_keys[3], D, D, 2.5),
        "w_gate": draw_weight(weight_keys[4], D, FF, 1.0),
        "w_up": draw_weight(weight_keys[5], D, FF, 1.0),
        "w_down": draw_weight(weight_keys[6], FF, D, 2.0),
    }


def layer_norm(values_bf):
    values = values_bf.astype(jnp.float32)
    mean_val = jnp.mean(values, axis=-1, keepdims=True)
    var_val = jnp.mean(values * values, axis=-1, keepdims=True) - mean_val * mean_val
    return ((values - mean_val) * lax.rsqrt(var_val + EPS)).astype(jnp.bfloat16)


def rotary(heads_bf):
    seq_len = heads_bf.shape[1]
    half_dim = HEAD_DIM // 2
    inv_freq = THETA ** (-2.0 * jnp.arange(half_dim, dtype=jnp.float32) / HEAD_DIM)
    angles = jnp.arange(seq_len, dtype=jnp.float32)[:, None] * inv_freq[None, :]
    cos_t = jnp.cos(angles)[:, None, :]
    sin_t = jnp.sin(angles)[:, None, :]
    values = heads_bf.astype(jnp.float32)
    lower_half = values[..., :half_dim]
    upper_half = values[..., half_dim:]
    return jnp.concatenate([lower_half * cos_t - upper_half * sin_t, upper_half * cos_t + lower_half * sin_t], axis=-1).astype(jnp.bfloat16)


def causal_attention(q_heads, k_heads, v_heads):
    seq_len = q_heads.shape[1]
    q_block = min(seq_len, 128)
    key_pos = jnp.arange(seq_len)
    k_vals = k_heads.astype(jnp.float32)
    v_vals = v_heads.astype(jnp.float32)

    def one_block(block_idx, out_acc):
        q_start = block_idx * q_block
        q_blk = lax.dynamic_slice_in_dim(q_heads, q_start, q_block, axis=1).astype(jnp.float32)
        scores = jnp.einsum("nqhd,nkhd->nhqk", q_blk, k_vals) * HEAD_DIM ** -0.5
        q_pos = q_start + jnp.arange(q_block)
        allowed = q_pos[:, None] >= key_pos[None, :]
        scores = jnp.where(allowed, scores, -1e30)
        prob_blk = jax.nn.softmax(scores, axis=-1).astype(jnp.bfloat16).astype(jnp.float32)
        blk_out = jnp.einsum("nhqk,nkhd->nqhd", prob_blk, v_vals).astype(jnp.bfloat16)
        return lax.dynamic_update_slice_in_dim(out_acc, blk_out, q_start, axis=1)

    return lax.fori_loop(0, seq_len // q_block, one_block, jnp.zeros_like(q_heads))


def project(rows_bf, weight):
    return jnp.dot(rows_bf, weight, preferred_element_type=jnp.float32).astype(jnp.bfloat16)


def reference(x_in, w_q, w_k, w_v, w_o, w_gate, w_up, w_down):
    n_seqs, seq_len, d_model = x_in.shape
    head_shape = (n_seqs, seq_len, HEADS, HEAD_DIM)
    x_rows = x_in.reshape(n_seqs * seq_len, d_model)
    normed = layer_norm(x_rows)
    q_heads = rotary(project(normed, w_q).reshape(head_shape))
    k_heads = rotary(project(normed, w_k).reshape(head_shape))
    v_heads = project(normed, w_v).reshape(head_shape)
    attn_heads = causal_attention(q_heads, k_heads, v_heads)
    attn_out = project(attn_heads.reshape(n_seqs * seq_len, d_model), w_o)
    resid_h = (x_rows.astype(jnp.float32) + attn_out.astype(jnp.float32)).astype(jnp.bfloat16)
    normed_mlp = layer_norm(resid_h)
    gate_val = project(normed_mlp, w_gate)
    up_val = project(normed_mlp, w_up)
    act_val = (jax.nn.silu(gate_val.astype(jnp.float32)) * up_val.astype(jnp.float32)).astype(jnp.bfloat16)
    mlp_out = project(act_val, w_down)
    y_out = (resid_h.astype(jnp.float32) + mlp_out.astype(jnp.float32)).astype(jnp.bfloat16)
    return y_out.reshape(n_seqs, seq_len, d_model)
```

```python
import functools

import jax
import jax.numpy as jnp
from jax import lax
from jax.experimental import pallas as pl
from jax.experimental.pallas import tpu as pltpu
from jax.sharding import PartitionSpec as P

HEAD_DIM = 128
EPS = 1e-5
THETA = 10000.0
Q_BLOCK = 256


def rotary_tables(seq_len):
    half_dim = HEAD_DIM // 2
    inv_freq = THETA ** (-2.0 * jnp.arange(half_dim, dtype=jnp.float32) / HEAD_DIM)
    angles = jnp.arange(seq_len, dtype=jnp.float32)[:, None] * inv_freq[None, :]
    cos_t, sin_t = jnp.cos(angles), jnp.sin(angles)
    return jnp.concatenate([cos_t, cos_t], axis=1), jnp.concatenate([-sin_t, sin_t], axis=1)


def attention_kernel(qkv_ref, cos_ref, sin_ref, o_ref):
    seq_len = qkv_ref.shape[0]
    scale_qk = HEAD_DIM ** -0.5

    def rotate(values_bf, rows):
        values = values_bf.astype(jnp.float32)
        turned = values * cos_ref[rows, :] + pltpu.roll(values, HEAD_DIM // 2, 1) * sin_ref[rows, :]
        return turned.astype(jnp.bfloat16)

    k_rot = rotate(qkv_ref[:, HEAD_DIM:2 * HEAD_DIM], slice(0, seq_len))
    v_all = qkv_ref[:, 2 * HEAD_DIM:3 * HEAD_DIM]
    for blk in range(seq_len // Q_BLOCK):
        rows = slice(blk * Q_BLOCK, (blk + 1) * Q_BLOCK)
        keys = (blk + 1) * Q_BLOCK
        q_rot = rotate(qkv_ref[rows, :HEAD_DIM], rows)
        scores = lax.dot_general(q_rot, k_rot[:keys], (((1,), (1,)), ((), ())), preferred_element_type=jnp.float32) * scale_qk
        q_pos = blk * Q_BLOCK + lax.broadcasted_iota(jnp.int32, (Q_BLOCK, keys), 0)
        k_pos = lax.broadcasted_iota(jnp.int32, (Q_BLOCK, keys), 1)
        scores = jnp.where(q_pos >= k_pos, scores, -1e30)
        weights = jnp.exp(scores - jnp.max(scores, axis=-1, keepdims=True))
        probs = (weights * (1.0 / jnp.sum(weights, axis=-1, keepdims=True))).astype(jnp.bfloat16)
        o_ref[rows, :] = jnp.dot(probs, v_all[:keys], preferred_element_type=jnp.float32).astype(jnp.bfloat16)


def attention(qkv, cos_t, sin_t):
    seq_len = qkv.shape[0]
    return pl.pallas_call(
        attention_kernel,
        out_shape=jax.ShapeDtypeStruct((seq_len, HEAD_DIM), jnp.bfloat16),
        in_specs=[pl.BlockSpec(memory_space=pltpu.VMEM)] * 3,
        out_specs=pl.BlockSpec(memory_space=pltpu.VMEM),
        cost_estimate=pl.CostEstimate(flops=4 * seq_len * seq_len * HEAD_DIM, bytes_accessed=2 * 1024 * 1024, transcendentals=seq_len * seq_len),
        name="attention",
    )(qkv, cos_t, sin_t)


def layer_norm(values):
    mean_val = jnp.mean(values, axis=-1, keepdims=True)
    var_val = jnp.mean(values * values, axis=-1, keepdims=True) - mean_val * mean_val
    return ((values - mean_val) * lax.rsqrt(var_val + EPS)).astype(jnp.bfloat16)


def dot32(a, b):
    return jnp.dot(a, b, preferred_element_type=jnp.float32)


def solution(mesh):
    n_tx, n_ty, n_dp = mesh.shape["tx"], mesh.shape["ty"], mesh.shape["dp"]
    act_spec = P(("dp", "ty"), None, "tx")
    col_spec = P("tx", "ty")
    row_spec = P("ty", "tx")
    f32, bf16 = jnp.float32, jnp.bfloat16

    def tx_xor(v, k):
        return lax.ppermute(v, "tx", [(i, i ^ k) for i in range(n_tx)])

    def swap_dp(v):
        return lax.ppermute(v, "dp", [(0, 1), (1, 0)])

    def move_ty(v, step, sources):
        return lax.ppermute(v, "ty", [(j, j + step) for j in sources])

    def gather_tx(v):
        far = tx_xor(v, 2)
        return [v, tx_xor(v, 1), far, tx_xor(far, 1)]

    def layer_fn(x_blk, w_q, w_k, w_v, w_o, w_gate, w_up, w_down):
        dp_i, ty_i, tx_i = lax.axis_index("dp"), lax.axis_index("ty"), lax.axis_index("tx")
        x_own = x_blk[0]
        seq_len, width = x_own.shape

        def in_order(mine, other, axis):
            return jnp.where(dp_i == 0, jnp.concatenate([mine, other], axis), jnp.concatenate([other, mine], axis))

        def gather_ty(v):
            up, down = [v], [v]
            for s in range(1, n_ty):
                up.append(move_ty(up[-1], 1, range(s - 1, n_ty - 1)))
                down.append(move_ty(down[-1], -1, range(1, n_ty - s + 1)))
            return [jnp.where(ty_i + r < n_ty, down[r], up[n_ty - r]) for r in range(1, n_ty)]

        def gather_weight_ty(w):
            half = w.shape[0] // 2
            mine = lax.dynamic_slice_in_dim(w, dp_i * half, half, 0)
            return [w] + [in_order(b, swap_dp(b), 0) for b in gather_ty(mine)]

        def gather_weight_tx(w):
            half = w.shape[0] // 2
            far_half = tx_xor(lax.dynamic_slice_in_dim(w, dp_i * half, half, 0), 2)
            far = in_order(far_half, swap_dp(far_half), 0)
            return [w, tx_xor(w, 1), far, tx_xor(far, 1)]

        x_parts = gather_tx(x_own)
        normed = layer_norm(jnp.concatenate([p.astype(f32) for p in x_parts], axis=1))

        heads_of = [w.reshape(width, n_tx, HEAD_DIM) for w in (w_q, w_k, w_v)]

        def qkv_piece(k):
            return jnp.concatenate([lax.dynamic_slice_in_dim(w, tx_i ^ k, 1, 1)[:, 0] for w in heads_of], axis=1)

        qkv_own = jnp.concatenate([qkv_piece(0)] + [tx_xor(qkv_piece(k), k) for k in range(1, n_tx)], axis=0)
        wo_heads = w_o.reshape(n_tx, HEAD_DIM, width)
        wo_own = jnp.concatenate([lax.dynamic_slice_in_dim(wo_heads, tx_i ^ k, 1, 0)[0] for k in range(n_tx)], axis=0)

        qkv_w = gather_weight_ty(qkv_own)
        wo_w = gather_weight_ty(wo_own)
        cos_t, sin_t = rotary_tables(seq_len)
        o_parts = []
        for r in range(n_ty):
            o_head = attention(dot32(normed, qkv_w[r]).astype(bf16), cos_t, sin_t)
            o_parts += gather_tx(o_head)
        attn_out = dot32(jnp.concatenate(o_parts, axis=1), jnp.concatenate(wo_w, axis=0)).astype(bf16)
        resid_h = (x_own.astype(f32) + attn_out.astype(f32)).astype(bf16)

        gate_all = jnp.concatenate(gather_weight_tx(w_gate), axis=0)
        up_all = jnp.concatenate(gather_weight_tx(w_up), axis=0)
        down_all = jnp.concatenate(gather_weight_tx(w_down), axis=1)

        quarter = seq_len // n_tx

        def h_piece(k):
            return lax.dynamic_slice_in_dim(resid_h, (tx_i ^ k) * quarter, quarter, 0)

        h_rows = jnp.concatenate([h_piece(0)] + [tx_xor(h_piece(k), k) for k in range(1, n_tx)], axis=1)
        normed_mlp = layer_norm(h_rows.astype(f32))

        n_chunks = 2
        chunk = quarter // n_chunks
        pieces = [[] for _ in range(n_tx)]
        for c in range(n_chunks):
            own = normed_mlp[c * chunk:(c + 1) * chunk]
            rows = jnp.concatenate([own] + gather_ty(own), axis=0)
            gate_val = dot32(rows, gate_all).astype(bf16).astype(f32)
            up_val = dot32(rows, up_all).astype(bf16).astype(f32)
            act_val = (jax.nn.silu(gate_val) * up_val).astype(bf16)
            part = dot32(act_val, down_all).astype(bf16)
            parts = [part[r * chunk:(r + 1) * chunk] for r in range(n_ty)]
            up = move_ty(parts[3], 1, [0])
            up = move_ty(parts[2] + up, 1, [0, 1])
            up = move_ty(parts[1] + up, 1, [0, 1, 2])
            dn = move_ty(parts[1], -1, [3])
            dn = move_ty(parts[2] + dn, -1, [3, 2])
            dn = move_ty(parts[3] + dn, -1, [3, 2, 1])
            total = (parts[0].astype(f32) + up.astype(f32) + dn.astype(f32)).astype(bf16)
            for k in range(n_tx):
                piece = total[:, k * width:(k + 1) * width]
                pieces[k].append(tx_xor(piece, k) if k else piece)
        mlp_out = jnp.zeros((seq_len, width), bf16)
        for k in range(n_tx):
            mlp_out = lax.dynamic_update_slice_in_dim(mlp_out, jnp.concatenate(pieces[k], axis=0), (tx_i ^ k) * quarter, 0)
        return (resid_h.astype(f32) + mlp_out.astype(f32)).astype(bf16)[None]

    return jax.shard_map(layer_fn, mesh=mesh, in_specs=(act_spec, col_spec, col_spec, col_spec, row_spec, col_spec, col_spec, row_spec), out_specs=act_spec, check_vma=False)
```

```python
import functools

import jax
import jax.numpy as jnp
from jax import lax
from jax.experimental import pallas as pl
from jax.experimental.pallas import tpu as pltpu
from jax.sharding import PartitionSpec as P

HEAD_DIM = 128
EPS = 1e-5
THETA = 10000.0
Q_BLOCK = 256


def rotary_tables(seq_len):
    half_dim = HEAD_DIM // 2
    inv_freq = THETA ** (-2.0 * jnp.arange(half_dim, dtype=jnp.float32) / HEAD_DIM)
    angles = jnp.arange(seq_len, dtype=jnp.float32)[:, None] * inv_freq[None, :]
    cos_t, sin_t = jnp.cos(angles), jnp.sin(angles)
    return jnp.concatenate([cos_t, cos_t], axis=1), jnp.concatenate([-sin_t, sin_t], axis=1)


def attention_kernel(qkv_ref, cos_ref, sin_ref, o_ref):
    seq_len = qkv_ref.shape[0]
    scale_qk = HEAD_DIM ** -0.5

    def rotate(values_bf, rows):
        values = values_bf.astype(jnp.float32)
        turned = values * cos_ref[rows, :] + pltpu.roll(values, HEAD_DIM // 2, 1) * sin_ref[rows, :]
        return turned.astype(jnp.bfloat16)

    k_rot = rotate(qkv_ref[:, HEAD_DIM:2 * HEAD_DIM], slice(0, seq_len))
    v_all = qkv_ref[:, 2 * HEAD_DIM:3 * HEAD_DIM]
    for blk in range(seq_len // Q_BLOCK):
        rows = slice(blk * Q_BLOCK, (blk + 1) * Q_BLOCK)
        keys = (blk + 1) * Q_BLOCK
        q_rot = rotate(qkv_ref[rows, :HEAD_DIM], rows)
        scores = lax.dot_general(q_rot, k_rot[:keys], (((1,), (1,)), ((), ())), preferred_element_type=jnp.float32) * scale_qk
        q_pos = blk * Q_BLOCK + lax.broadcasted_iota(jnp.int32, (Q_BLOCK, keys), 0)
        k_pos = lax.broadcasted_iota(jnp.int32, (Q_BLOCK, keys), 1)
        scores = jnp.where(q_pos >= k_pos, scores, -1e30)
        weights = jnp.exp(scores - jnp.max(scores, axis=-1, keepdims=True))
        probs = (weights * (1.0 / jnp.sum(weights, axis=-1, keepdims=True))).astype(jnp.bfloat16)
        o_ref[rows, :] = jnp.dot(probs, v_all[:keys], preferred_element_type=jnp.float32).astype(jnp.bfloat16)


def attention(qkv, cos_t, sin_t):
    seq_len = qkv.shape[0]
    return pl.pallas_call(
        attention_kernel,
        out_shape=jax.ShapeDtypeStruct((seq_len, HEAD_DIM), jnp.bfloat16),
        in_specs=[pl.BlockSpec(memory_space=pltpu.VMEM)] * 3,
        out_specs=pl.BlockSpec(memory_space=pltpu.VMEM),
        cost_estimate=pl.CostEstimate(flops=4 * seq_len * seq_len * HEAD_DIM, bytes_accessed=2 * 1024 * 1024, transcendentals=seq_len * seq_len),
        name="attention",
    )(qkv, cos_t, sin_t)


def layer_norm(values):
    mean_val = jnp.mean(values, axis=-1, keepdims=True)
    var_val = jnp.mean(values * values, axis=-1, keepdims=True) - mean_val * mean_val
    return ((values - mean_val) * lax.rsqrt(var_val + EPS)).astype(jnp.bfloat16)


N_TILE = 256
CHUNKS = 4


def mlp_kernel(n_ty, n_tx, chunks, h_ref, *refs):
    weight_refs, (y_ref, gate_v, up_v, down_v, h_rows, n_buf, act_v, part, from_low, from_high, y_in, w_sem, a_send, a_recv, g_send, g_recv, s_send, lo_recv, hi_recv, o_send, o_recv) = refs[:3 * n_tx], refs[3 * n_tx:]
    z, i = lax.axis_index("ty"), lax.axis_index("tx")
    seq_len, width = h_ref.shape
    quarter = seq_len // n_tx
    ch = quarter // chunks
    full = n_tx * width
    ff = gate_v.shape[1]
    f32, bf16 = jnp.float32, jnp.bfloat16
    last = n_ty - 1

    weight_copies = []
    for k in range(n_tx):
        span = pl.ds(k * width, width)
        weight_copies += [
            pltpu.make_async_copy(weight_refs[k], gate_v.at[span], w_sem.at[k]),
            pltpu.make_async_copy(weight_refs[n_tx + k], up_v.at[span], w_sem.at[n_tx + k]),
            pltpu.make_async_copy(weight_refs[2 * n_tx + k], down_v.at[:, span], w_sem.at[2 * n_tx + k]),
        ]
    for copy in weight_copies:
        copy.start()

    barrier = pltpu.get_barrier_semaphore()
    for k in range(1, n_tx):
        pl.semaphore_signal(barrier, inc=1, device_id={"tx": i ^ k}, device_id_type=pl.DeviceIdType.MESH)

    @pl.when(z > 0)
    def _():
        pl.semaphore_signal(barrier, inc=1, device_id={"ty": z - 1}, device_id_type=pl.DeviceIdType.MESH)

    @pl.when(z < last)
    def _():
        pl.semaphore_signal(barrier, inc=1, device_id={"ty": z + 1}, device_id_type=pl.DeviceIdType.MESH)

    @pl.when((z > 0) & (z < last))
    def _():
        pl.semaphore_wait(barrier, n_tx + 1)

    @pl.when((z == 0) | (z == last))
    def _():
        pl.semaphore_wait(barrier, n_tx)

    def remote(src, dst, send, recv, where):
        return pltpu.make_async_remote_copy(src_ref=src, dst_ref=dst, send_sem=send, recv_sem=recv, device_id=where, device_id_type=pl.DeviceIdType.MESH)

    def spread(c, k):
        rows = pl.ds(pl.multiple_of((i ^ k) * quarter + c * ch, ch), ch)
        return remote(h_ref.at[rows], h_rows.at[c, :, pl.ds(k * width, width)], a_send.at[c, k], a_recv.at[c, k], {"tx": i ^ k})

    def gather(c, src, step):
        return remote(n_buf.at[c, src], n_buf.at[c, src], g_send.at[c, src, (step + 1) // 2], g_recv.at[c, src], {"ty": z + step})

    def reduce(c, dst, step):
        landing, sems = (from_low, lo_recv) if step == 1 else (from_high, hi_recv)
        return remote(part.at[c, dst], landing.at[c, dst], s_send.at[c, dst], sems.at[c, dst], {"ty": z + step})

    def collect(c, k):
        rows = pl.ds(pl.multiple_of(i * quarter + c * ch, ch), ch)
        return remote(part.at[c, z, :, pl.ds(k * width, width)], y_in.at[rows], o_send.at[c, k], o_recv.at[c, k], {"tx": i ^ k})

    for c in range(chunks):
        for k in range(1, n_tx):
            spread(c, k).start()

    def norm_chunk(c):
        for k in range(1, n_tx):
            spread(c, k).wait_recv()
        own = pl.ds(pl.multiple_of(i * quarter + c * ch, ch), ch)
        h_rows[c, :, :width] = h_ref[own, :]
        block = min(ch, 32)
        for b in range(ch // block):
            rows = slice(b * block, (b + 1) * block)
            n_buf[c, z, rows, :] = layer_norm(h_rows[c, rows, :].astype(f32))

    def gather_own(c):
        @pl.when(z < last)
        def _():
            gather(c, z, 1).start()

        @pl.when(z > 0)
        def _():
            gather(c, z, -1).start()

    def gather_hop(c, hop):
        @pl.when(z >= hop)
        def _():
            gather(c, z - hop, 1).wait_recv()

            @pl.when(z < last)
            def _():
                gather(c, z - hop, 1).start()

        @pl.when(z + hop <= last)
        def _():
            gather(c, z + hop, -1).wait_recv()

            @pl.when(z > 0)
            def _():
                gather(c, z + hop, -1).start()

    def compute(c, third):
        n_tiles, d_tiles = ff // N_TILE, full // N_TILE
        steps = n_tiles + d_tiles
        lo, hi = steps * third // 3, steps * (third + 1) // 3

        def gate_up(t, carry):
            cols = pl.ds(pl.multiple_of(t * N_TILE, N_TILE), N_TILE)
            rows = n_buf[c].reshape(n_ty * ch, full)
            gate_val = jnp.dot(rows, gate_v[:, cols], preferred_element_type=f32).astype(bf16).astype(f32)
            up_val = jnp.dot(rows, up_v[:, cols], preferred_element_type=f32).astype(bf16).astype(f32)
            act_v[:, cols] = (gate_val * jax.nn.sigmoid(gate_val) * up_val).astype(bf16)
            return carry

        def down(t, carry):
            cols = pl.ds(pl.multiple_of(t * N_TILE, N_TILE), N_TILE)
            out = jnp.dot(act_v[...], down_v[:, cols], preferred_element_type=f32).astype(bf16)
            part[c, :, :, cols] = out.reshape(n_ty, ch, N_TILE)
            return carry

        if lo < n_tiles:
            lax.fori_loop(lo, min(hi, n_tiles), gate_up, 0)
        if hi > n_tiles:
            lax.fori_loop(max(lo, n_tiles) - n_tiles, hi - n_tiles, down, 0)

    def add_into(c, dst, landing):
        part[c, dst] = (part[c, dst].astype(f32) + landing[c, dst].astype(f32)).astype(bf16)

    def reduce_hop(c, hop):
        dist = n_ty - hop

        @pl.when(z + dist <= last)
        def _():
            @pl.when(z > 0)
            def _():
                reduce(c, z + dist, 1).wait_recv()
                add_into(c, z + dist, from_low)

            reduce(c, z + dist, 1).start()

        @pl.when(z >= dist)
        def _():
            @pl.when(z < last)
            def _():
                reduce(c, z - dist, -1).wait_recv()
                add_into(c, z - dist, from_high)

            reduce(c, z - dist, -1).start()

    def reduce_end(c):
        @pl.when(z > 0)
        def _():
            reduce(c, z, 1).wait_recv()

        @pl.when(z < last)
        def _():
            reduce(c, z, -1).wait_recv()

        @pl.when(z == 0)
        def _():
            add_into(c, z, from_high)

        @pl.when(z == last)
        def _():
            add_into(c, z, from_low)

        @pl.when((z > 0) & (z < last))
        def _():
            total = part[c, z].astype(f32) + from_low[c, z].astype(f32) + from_high[c, z].astype(f32)
            part[c, z] = total.astype(bf16)

        for k in range(1, n_tx):
            collect(c, k).start()
        rows = pl.ds(pl.multiple_of(i * quarter + c * ch, ch), ch)
        y_in[rows, :] = part[c, z, :, :width]

    norm_chunk(0)
    gather_own(0)
    for c in range(1, chunks):
        norm_chunk(c)
    for t in range(chunks + 2):
        if 0 < t < chunks:
            gather_own(t)
        if t == 1:
            for copy in weight_copies:
                copy.wait()
        for hop in range(1, n_ty):
            if t >= 2:
                reduce_hop(t - 2, hop)
            if 1 <= t <= chunks:
                compute(t - 1, hop - 1)
            if t < chunks:
                gather_hop(t, hop)
        if t >= 2:
            reduce_end(t - 2)

    for c in range(chunks):
        for k in range(1, n_tx):
            collect(c, k).wait_recv()
    for b in range(8):
        rows = slice(b * seq_len // 8, (b + 1) * seq_len // 8)
        y_ref[rows, :] = (h_ref[rows, :].astype(f32) + y_in[rows, :].astype(f32)).astype(bf16)

    for c in range(chunks):
        for k in range(1, n_tx):
            spread(c, k).wait_send()
            collect(c, k).wait_send()
        for src in range(n_ty):
            @pl.when((z >= src) & (z < last))
            def _():
                gather(c, src, 1).wait_send()

            @pl.when((z <= src) & (z > 0))
            def _():
                gather(c, src, -1).wait_send()

            @pl.when(z < src)
            def _():
                reduce(c, src, 1).wait_send()

            @pl.when(z > src)
            def _():
                reduce(c, src, -1).wait_send()


def mlp_fused(resid_h, gates, ups, downs, n_ty):
    seq_len, width = resid_h.shape
    n_tx = len(gates)
    full, ff = n_tx * width, gates[0].shape[1]
    chunks = CHUNKS
    ch = seq_len // n_tx // chunks
    bf16 = jnp.bfloat16
    dma = pltpu.SemaphoreType.DMA
    return pl.pallas_call(
        functools.partial(mlp_kernel, n_ty, n_tx, chunks),
        out_shape=jax.ShapeDtypeStruct((seq_len, width), bf16),
        in_specs=[pl.BlockSpec(memory_space=pltpu.VMEM)] + [pl.BlockSpec(memory_space=pl.ANY)] * (3 * n_tx),
        out_specs=pl.BlockSpec(memory_space=pltpu.VMEM),
        scratch_shapes=[
            pltpu.VMEM((full, ff), bf16),
            pltpu.VMEM((full, ff), bf16),
            pltpu.VMEM((ff, full), bf16),
            pltpu.VMEM((chunks, ch, full), bf16),
            pltpu.VMEM((chunks, n_ty, ch, full), bf16),
            pltpu.VMEM((n_ty * ch, ff), bf16),
            pltpu.VMEM((chunks, n_ty, ch, full), bf16),
            pltpu.VMEM((chunks, n_ty, ch, full), bf16),
            pltpu.VMEM((chunks, n_ty, ch, full), bf16),
            pltpu.VMEM((seq_len, width), bf16),
            dma((3 * n_tx,)),
            dma((chunks, n_tx)), dma((chunks, n_tx)),
            dma((chunks, n_ty, 2)), dma((chunks, n_ty)),
            dma((chunks, n_ty)), dma((chunks, n_ty)), dma((chunks, n_ty)),
            dma((chunks, n_tx)), dma((chunks, n_tx)),
        ],
        compiler_params=pltpu.CompilerParams(collective_id=1, has_side_effects=True, vmem_limit_bytes=62 * 1024 * 1024),
        cost_estimate=pl.CostEstimate(flops=6 * seq_len * full * ff, bytes_accessed=6 * full * ff, transcendentals=seq_len * ff),
        name="mlp_fused",
    )(resid_h, *gates, *ups, *downs)


def dot32(a, b):
    return jnp.dot(a, b, preferred_element_type=jnp.float32)


def solution(mesh):
    n_tx, n_ty, n_dp = mesh.shape["tx"], mesh.shape["ty"], mesh.shape["dp"]
    act_spec = P(("dp", "ty"), None, "tx")
    col_spec = P("tx", "ty")
    row_spec = P("ty", "tx")
    f32, bf16 = jnp.float32, jnp.bfloat16

    def tx_xor(v, k):
        return lax.ppermute(v, "tx", [(i, i ^ k) for i in range(n_tx)])

    def swap_dp(v):
        return lax.ppermute(v, "dp", [(0, 1), (1, 0)])

    def move_ty(v, step, sources):
        return lax.ppermute(v, "ty", [(j, j + step) for j in sources])

    def gather_tx(v):
        far = tx_xor(v, 2)
        return [v, tx_xor(v, 1), far, tx_xor(far, 1)]

    def layer_fn(x_blk, w_q, w_k, w_v, w_o, w_gate, w_up, w_down):
        dp_i, ty_i, tx_i = lax.axis_index("dp"), lax.axis_index("ty"), lax.axis_index("tx")
        x_own = x_blk[0]
        seq_len, width = x_own.shape

        def in_order(mine, other, axis):
            return jnp.where(dp_i == 0, jnp.concatenate([mine, other], axis), jnp.concatenate([other, mine], axis))

        def gather_ty(v):
            up, down = [v], [v]
            for s in range(1, n_ty):
                up.append(move_ty(up[-1], 1, range(s - 1, n_ty - 1)))
                down.append(move_ty(down[-1], -1, range(1, n_ty - s + 1)))
            return [jnp.where(ty_i + r < n_ty, down[r], up[n_ty - r]) for r in range(1, n_ty)]

        def gather_weight_ty(w):
            half = w.shape[0] // 2
            mine = lax.dynamic_slice_in_dim(w, dp_i * half, half, 0)
            return [w] + [in_order(b, swap_dp(b), 0) for b in gather_ty(mine)]

        def gather_weight_tx(w):
            half = w.shape[0] // 2
            far_half = tx_xor(lax.dynamic_slice_in_dim(w, dp_i * half, half, 0), 2)
            far = in_order(far_half, swap_dp(far_half), 0)
            return [w, tx_xor(w, 1), far, tx_xor(far, 1)]

        x_parts = gather_tx(x_own)
        normed = layer_norm(jnp.concatenate([p.astype(f32) for p in x_parts], axis=1))

        def qkv_piece(k):
            return jnp.concatenate([lax.dynamic_slice_in_dim(w, (tx_i ^ k) * HEAD_DIM, HEAD_DIM, 1) for w in (w_q, w_k, w_v)], axis=1)

        qkv_own = jnp.concatenate([qkv_piece(0)] + [tx_xor(qkv_piece(k), k) for k in range(1, n_tx)], axis=0)
        wo_heads = w_o.reshape(n_tx, HEAD_DIM, width)
        wo_own = jnp.concatenate([lax.dynamic_slice_in_dim(wo_heads, tx_i ^ k, 1, 0)[0] for k in range(n_tx)], axis=0)

        qkv_w = gather_weight_ty(qkv_own)
        wo_w = gather_weight_ty(wo_own)
        cos_t, sin_t = rotary_tables(seq_len)
        o_parts = []
        for r in range(n_ty):
            o_head = attention(dot32(normed, qkv_w[r]).astype(bf16), cos_t, sin_t)
            o_parts += gather_tx(o_head)
        attn_out = dot32(jnp.concatenate(o_parts, axis=1), jnp.concatenate(wo_w, axis=0)).astype(bf16)
        resid_h = (x_own.astype(f32) + attn_out.astype(f32)).astype(bf16)

        gates, ups, downs = gather_weight_tx(w_gate), gather_weight_tx(w_up), gather_weight_tx(w_down)
        return mlp_fused(resid_h, gates, ups, downs, n_ty)[None]

    return jax.shard_map(layer_fn, mesh=mesh, in_specs=(act_spec, col_spec, col_spec, col_spec, row_spec, col_spec, col_spec, row_spec), out_specs=act_spec, check_vma=False)
```

```python
import functools

import jax
import jax.numpy as jnp
from jax import lax
from jax.experimental import pallas as pl
from jax.experimental.pallas import tpu as pltpu
from jax.sharding import PartitionSpec as P

HEAD_DIM = 128
EPS = 1e-5
THETA = 10000.0
Q_BLOCK = 256
N_TILE = 256
CHUNKS = 4
N_TX = 4
N_TY = 4

f32, bf16 = jnp.float32, jnp.bfloat16


def rotary_tables(seq_len):
    half_dim = HEAD_DIM // 2
    inv_freq = THETA ** (-2.0 * jnp.arange(half_dim, dtype=jnp.float32) / HEAD_DIM)
    angles = jnp.arange(seq_len, dtype=jnp.float32)[:, None] * inv_freq[None, :]
    cos_t, sin_t = jnp.cos(angles), jnp.sin(angles)
    return jnp.concatenate([cos_t, cos_t], axis=1), jnp.concatenate([-sin_t, sin_t], axis=1)


def layer_norm(values):
    mean_val = jnp.mean(values, axis=-1, keepdims=True)
    var_val = jnp.mean(values * values, axis=-1, keepdims=True) - mean_val * mean_val
    return ((values - mean_val) * lax.rsqrt(var_val + EPS)).astype(bf16)


def layer_kernel(x_ref, wq_ref, wk_ref, wv_ref, wo_ref, wg_ref, wu_ref, wd_ref, cos_ref, sin_ref, y_ref,
                 x_all, w_all, wo_all, qkv_v, o_all, h_v, gate_v, up_v, down_v, h_rows, n_buf, act_v, work, landing, landing2, y_in,
                 loc_sem, x_send, x_recv, q_send, q_recv, z_send, z_recv, zx_send, zx_recv, p_send, p_recv, px_send, px_recv,
                 og_send, og_recv, m1_send, m1_recv, my_send, my_recv, mx_send, mx_recv, mf_send, mf_recv,
                 a_send, a_recv, g_send, g_recv, s_send, lo_recv, hi_recv, c_send, c_recv):
    d, z, i = lax.axis_index("dp"), lax.axis_index("ty"), lax.axis_index("tx")
    yy, core = i // 2, i % 2
    n_tx, n_ty, chunks = N_TX, N_TY, CHUNKS
    seq_len, width = x_ref.shape
    full, ff = n_tx * width, gate_v.shape[1]
    quarter = seq_len // n_tx
    ch = quarter // chunks
    half_w = width // 2
    last = n_ty - 1
    MESH = pl.DeviceIdType.MESH

    def tx_to(k):
        return {"tx": i ^ k}

    def remote(src, dst, send, recv, where):
        return pltpu.make_async_remote_copy(src_ref=src, dst_ref=dst, send_sem=send, recv_sem=recv, device_id=where, device_id_type=MESH)

    def aligned(v, m):
        return pl.multiple_of(v, m)

    x_half = seq_len // 2

    def x_copy(c, k):
        rows = pl.ds(c * x_half, x_half)
        if k == 3:
            return remote(x_all.at[i ^ 2, rows], x_all.at[i ^ 2, rows], x_send.at[c, 3], x_recv.at[c, 3], tx_to(1))
        return remote(x_ref.at[rows], x_all.at[i, rows], x_send.at[c, k], x_recv.at[c, k], tx_to(k))

    mats = (wq_ref, wk_ref, wv_ref)

    def q_copy(k, m, h):
        src = mats[m].at[pl.ds(aligned(h * half_w, half_w), half_w), pl.ds(aligned((i ^ k) * HEAD_DIM, HEAD_DIM), HEAD_DIM)]
        dst = w_all.at[z, h, yy, pl.ds(aligned(core * half_w, half_w), half_w), pl.ds(m * HEAD_DIM, HEAD_DIM)]
        if k == 0:
            return pltpu.make_async_copy(src, dst, q_recv.at[0, m, h])
        return remote(src, dst, q_send.at[k, m, h], q_recv.at[k, m, h], tx_to(k))

    def chip_of(g):
        return yy if g == 0 else 1 - yy

    def z_copy(src, g, step):
        block = w_all.at[src, d, chip_of(g)]
        return remote(block, block, z_send.at[src, g, (step + 1) // 2], z_recv.at[src, g], {"ty": z + step})

    def zx_copy(src, g):
        block = w_all.at[src, d, chip_of(g)]
        return remote(block, block, zx_send.at[src, g], zx_recv.at[src, g], {"dp": 1 - d})

    def p_rows():
        return pl.ds(aligned(d * half_w, half_w), half_w)

    def p_copy(src, step):
        block = wo_all.at[src, p_rows()]
        return remote(block, block, p_send.at[src, (step + 1) // 2], p_recv.at[src], {"ty": z + step})

    def px_copy(src):
        block = wo_all.at[src, p_rows()]
        return remote(block, block, px_send.at[src], px_recv.at[src], {"dp": 1 - d})

    def og_copy(src, k):
        head = (i ^ 2) if k == 3 else i
        block = o_all.at[:, pl.ds(aligned(src * width + head * HEAD_DIM, HEAD_DIM), HEAD_DIM)]
        return remote(block, block, og_send.at[src, k], og_recv.at[src, k], tx_to(1 if k == 3 else k))

    own_w, full_w = (wg_ref, wu_ref, wd_ref), (gate_v, up_v, down_v)
    q_rows = (half_w // 2, half_w // 2, ff // 4)

    def m_span(a, h, q):
        return pl.ds(aligned((h * 2 + q) * q_rows[a], q_rows[a]), q_rows[a])

    def m_slot(a, k, h, q):
        if a == 2:
            return down_v.at[m_span(a, h, q), pl.ds(k * width, width)]
        return full_w[a].at[pl.ds(aligned(k * width + (h * 2 + q) * q_rows[a], q_rows[a]), q_rows[a])]

    def m_block(a, k):
        if a == 2:
            return down_v.at[:, pl.ds(k * width, width)]
        return full_w[a].at[pl.ds(k * width, width)]

    def m_own(a):
        return pltpu.make_async_copy(own_w[a], m_block(a, 0), loc_sem.at[a])

    def m_near(a):
        return remote(own_w[a], m_block(a, 1), m1_send.at[a], m1_recv.at[a], tx_to(1))

    def m_far(a, q):
        return remote(own_w[a].at[m_span(a, d, q)], m_slot(a, 2, d, q), my_send.at[a, q], my_recv.at[a, q], tx_to(2))

    def m_swap(a, q):
        return remote(m_slot(a, 2, d, q), m_slot(a, 2, d, q), mx_send.at[a, q], mx_recv.at[a, q], {"dp": 1 - d})

    def m_pass(a, q, h):
        return remote(m_slot(a, 2, h, q), m_slot(a, 3, h, q), mf_send.at[a, q, h], mf_recv.at[a, q, h], tx_to(1))

    PIECES = [(a, q) for a in range(3) for q in range(2)]

    def m_far_start(p):
        m_far(*PIECES[p]).start()

    def m_far_done(p):
        a, q = PIECES[p]
        m_far(a, q).wait_recv()
        m_swap(a, q).start()
        m_pass(a, q, d).start()

    def m_swap_done(p):
        a, q = PIECES[p]
        m_swap(a, q).wait_recv()
        m_pass(a, q, 1 - d).start()

    def m_ready(a):
        m_own(a).wait()
        m_near(a).wait_recv()
        for q in range(2):
            for h in range(2):
                m_pass(a, q, h).wait_recv()

    def slot(c, dst):
        return pl.ds(aligned((c * n_ty + dst) * ch, ch), ch)

    def own_rows(c):
        return pl.ds(aligned(i * quarter + c * ch, ch), ch)

    def spread(c, k):
        rows = pl.ds(aligned((i ^ k) * quarter + c * ch, ch), ch)
        return remote(h_v.at[rows], h_rows.at[c, :, pl.ds(k * width, width)], a_send.at[c, k], a_recv.at[c, k], tx_to(k))

    def gather(c, src, step):
        return remote(n_buf.at[c, src], n_buf.at[c, src], g_send.at[c, src, (step + 1) // 2], g_recv.at[c, src], {"ty": z + step})

    def reduce(c, dst, step, final):
        src = work.at[slot(c, dst)]
        if step == 1:
            return remote(src, landing.at[slot(c, dst)], s_send.at[c, dst], lo_recv.at[c, dst], {"ty": z + 1})
        if final:
            return remote(src, landing2.at[c], s_send.at[c, dst], hi_recv.at[c, 0], {"ty": z - 1})
        return remote(src, landing.at[slot(c, dst)], s_send.at[c, dst], lo_recv.at[c, dst], {"ty": z - 1})

    def collect(c, k):
        return remote(work.at[slot(c, z), pl.ds(k * width, width)], y_in.at[own_rows(c)], c_send.at[c, k], c_recv.at[c, k], tx_to(k))

    x_own = pltpu.make_async_copy(x_ref, x_all.at[i], loc_sem.at[3])
    wo_own = pltpu.make_async_copy(wo_ref, wo_all.at[z], loc_sem.at[4])
    for m in range(3):
        for h in range(2):
            q_copy(0, m, h).start()
    x_own.start()
    wo_own.start()

    barrier = pltpu.get_barrier_semaphore()
    for k in range(1, n_tx):
        pl.semaphore_signal(barrier, inc=1, device_id=tx_to(k), device_id_type=MESH)
    pl.semaphore_signal(barrier, inc=1, device_id={"dp": 1 - d}, device_id_type=MESH)

    @pl.when(z > 0)
    def _():
        pl.semaphore_signal(barrier, inc=1, device_id={"ty": z - 1}, device_id_type=MESH)

    @pl.when(z < last)
    def _():
        pl.semaphore_signal(barrier, inc=1, device_id={"ty": z + 1}, device_id_type=MESH)

    @pl.when((z > 0) & (z < last))
    def _():
        pl.semaphore_wait(barrier, n_tx + 2)

    @pl.when((z == 0) | (z == last))
    def _():
        pl.semaphore_wait(barrier, n_tx + 1)

    for m in range(3):
        q_copy(1, m, d).start()
    for k in (2, 3):
        for m in range(3):
            q_copy(k, m, d).start()
    for m in range(3):
        q_copy(1, m, 1 - d).start()
    for c in range(2):
        x_copy(c, 1).start()
    for c in range(2):
        x_copy(c, 2).start()
    for k in (2, 3):
        for m in range(3):
            q_copy(k, m, 1 - d).start()
    for a in range(3):
        m_own(a).start()

    def both_ways(make):
        @pl.when(z < last)
        def _():
            make(1).start()

        @pl.when(z > 0)
        def _():
            make(-1).start()

    def hop(make, swap, h):
        @pl.when(z >= h)
        def _():
            make(z - h, 1).wait_recv()

            @pl.when(z < last)
            def _():
                make(z - h, 1).start()

            if swap is not None:
                swap(z - h).start()

        @pl.when(z + h <= last)
        def _():
            make(z + h, -1).wait_recv()

            @pl.when(z > 0)
            def _():
                make(z + h, -1).start()

            if swap is not None:
                swap(z + h).start()

    def z_hop(g, h):
        hop(lambda src, step: z_copy(src, g, step), lambda src: zx_copy(src, g), h)

    def p_hop(h):
        hop(p_copy, px_copy, h)

    def norm_rows(c):
        block = 32

        def body(t, carry):
            rows = pl.ds(aligned(c * x_half + t * block, block), block)
            parts = [x_all[j, rows, :].astype(f32) for j in range(n_tx)]
            normed = layer_norm(jnp.concatenate(parts, axis=1))
            for j in range(n_tx):
                for h in range(2):
                    to = h * (full // 2) + j * half_w
                    work[rows, to:to + half_w] = normed[:, j * width + h * half_w:j * width + (h + 1) * half_w]
            return carry

        lax.fori_loop(0, x_half // block, body, 0)

    s = z // 2
    order = [z, 1 - z + 4 * s, 2 - s, 3 - 3 * s]

    def project_heads(src):
        tile = 256

        def body(t, carry):
            rows = pl.ds(aligned(t * tile, tile), tile)
            weight = w_all[src].reshape(full, 3 * HEAD_DIM)
            qkv_v[rows, :] = jnp.dot(work[rows, :], weight, preferred_element_type=f32).astype(bf16)
            return carry

        lax.fori_loop(0, seq_len // tile, body, 0)

    def rotate(values_bf, rows):
        values = values_bf.astype(f32)
        turned = values * cos_ref[rows, :] + pltpu.roll(values, HEAD_DIM // 2, 1) * sin_ref[rows, :]
        return turned.astype(bf16)

    def attend(src):
        cols = pl.ds(aligned(src * width + i * HEAD_DIM, HEAD_DIM), HEAD_DIM)
        k_rot = rotate(qkv_v[:, HEAD_DIM:2 * HEAD_DIM], slice(0, seq_len))
        v_all = qkv_v[:, 2 * HEAD_DIM:3 * HEAD_DIM]
        for blk in range(seq_len // Q_BLOCK):
            rows = slice(blk * Q_BLOCK, (blk + 1) * Q_BLOCK)
            keys = (blk + 1) * Q_BLOCK
            q_rot = rotate(qkv_v[rows, :HEAD_DIM], rows)
            scores = lax.dot_general(q_rot, k_rot[:keys], (((1,), (1,)), ((), ())), preferred_element_type=f32) * HEAD_DIM ** -0.5
            q_pos = blk * Q_BLOCK + lax.broadcasted_iota(jnp.int32, (Q_BLOCK, keys), 0)
            k_pos = lax.broadcasted_iota(jnp.int32, (Q_BLOCK, keys), 1)
            scores = jnp.where(q_pos >= k_pos, scores, -1e30)
            weights = jnp.exp(scores - jnp.max(scores, axis=-1, keepdims=True))
            probs = (weights * (1.0 / jnp.sum(weights, axis=-1, keepdims=True))).astype(bf16)
            o_all[rows, cols] = jnp.dot(probs, v_all[:keys], preferred_element_type=f32).astype(bf16)

    def og_start(r):
        og_copy(order[r], 2).start()
        og_copy(order[r], 1).start()

    def og_pass(r):
        og_copy(order[r], 2).wait_recv()
        og_copy(order[r], 3).start()

    def block_ready(r):
        for g in range(2):
            zx_copy(order[r], g).wait_recv()

    for m in range(3):
        for h in range(2):
            q_copy(0, m, h).wait()
        q_copy(1, m, d).wait_recv()
    both_ways(lambda step: z_copy(z, 0, step))
    for k in (2, 3):
        for m in range(3):
            q_copy(k, m, d).wait_recv()
    both_ways(lambda step: z_copy(z, 1, step))
    wo_own.wait()
    z_hop(0, 1)
    x_own.wait()
    for c in range(2):
        x_copy(c, 1).wait_recv()
    x_copy(0, 2).wait_recv()
    x_copy(0, 3).start()
    z_hop(1, 1)
    x_copy(0, 3).wait_recv()
    norm_rows(0)
    z_hop(0, 2)
    x_copy(1, 2).wait_recv()
    x_copy(1, 3).start()
    m_far_start(0)
    m_near(0).start()
    x_copy(1, 3).wait_recv()
    norm_rows(1)
    z_hop(1, 2)
    both_ways(lambda step: p_copy(z, step))
    for m in range(3):
        q_copy(1, m, 1 - d).wait_recv()
        for k in (2, 3):
            q_copy(k, m, 1 - d).wait_recv()
    project_heads(order[0])
    z_hop(0, 3)
    attend(order[0])
    og_start(0)
    m_far_start(1)
    m_near(1).start()
    z_hop(1, 3)
    block_ready(1)
    project_heads(order[1])
    m_far_done(0)
    p_hop(1)
    og_pass(0)
    attend(order[1])
    og_start(1)
    m_far_start(2)
    p_hop(2)
    block_ready(2)
    project_heads(order[2])
    m_far_done(1)
    p_hop(3)
    og_pass(1)
    attend(order[2])
    og_start(2)
    m_near(2).start()
    block_ready(3)
    project_heads(order[3])
    m_far_done(2)
    attend(order[3])
    og_start(3)
    m_far_start(3)
    m_far_start(4)
    og_pass(2)
    m_swap_done(0)
    og_pass(3)
    for r in range(1, n_ty):
        px_copy(order[r]).wait_recv()
    for r in range(n_ty):
        og_copy(order[r], 1).wait_recv()
        og_copy(order[r], 3).wait_recv()

    def out_project(t, carry):
        rows = pl.ds(aligned(t * 256, 256), 256)
        attn_out = jnp.dot(o_all[rows, :], wo_all[...].reshape(full, width), preferred_element_type=f32).astype(bf16)
        h_v[rows, :] = (x_all[i, rows, :].astype(f32) + attn_out.astype(f32)).astype(bf16)
        return carry

    lax.fori_loop(0, seq_len // 256, out_project, 0)

    for c in range(chunks):
        for k in (2, 3, 1):
            spread(c, k).start()
    m_far_start(5)
    m_swap_done(1)
    m_far_done(3)

    def norm_chunk(c):
        for k in range(1, n_tx):
            spread(c, k).wait_recv()
        h_rows[c, :, :width] = h_v[own_rows(c), :]
        block = min(ch, 32)
        for b in range(ch // block):
            rows = slice(b * block, (b + 1) * block)
            n_buf[c, z, rows, :] = layer_norm(h_rows[c, rows, :].astype(f32))

    def gather_own(c):
        both_ways(lambda step: gather(c, z, step))

    def gather_hop(c, h):
        hop(lambda src, step: gather(c, src, step), None, h)

    n_tiles, d_tiles = ff // N_TILE, full // N_TILE

    def gate_up(c, lo, hi):
        def body(t, carry):
            cols = pl.ds(aligned(t * N_TILE, N_TILE), N_TILE)
            rows = n_buf[c].reshape(n_ty * ch, full)
            gate_val = jnp.dot(rows, gate_v[:, cols], preferred_element_type=f32).astype(bf16).astype(f32)
            up_val = jnp.dot(rows, up_v[:, cols], preferred_element_type=f32).astype(bf16).astype(f32)
            act_v[:, cols] = (gate_val * jax.nn.sigmoid(gate_val) * up_val).astype(bf16)
            return carry

        lax.fori_loop(lo, hi, body, 0)

    def down(c, lo, hi):
        def body(t, carry):
            cols = pl.ds(aligned(t * N_TILE, N_TILE), N_TILE)
            work[pl.ds(c * n_ty * ch, n_ty * ch), cols] = jnp.dot(act_v[...], down_v[:, cols], preferred_element_type=f32).astype(bf16)
            return carry

        lax.fori_loop(lo, hi, body, 0)

    def compute(c, third):
        steps = n_tiles + d_tiles
        lo, hi = steps * third // 3, steps * (third + 1) // 3
        if lo < n_tiles:
            gate_up(c, lo, min(hi, n_tiles))
        if hi > n_tiles:
            if c == 0 and lo <= n_tiles:
                m_swap_done(4)
                m_swap_done(5)
                m_ready(2)
            down(c, max(lo, n_tiles) - n_tiles, hi - n_tiles)

    def add_into(c, dst):
        work[slot(c, dst), :] = (work[slot(c, dst), :].astype(f32) + landing[slot(c, dst), :].astype(f32)).astype(bf16)

    def reduce_hop(c, h):
        dist = n_ty - h

        @pl.when(z + dist <= last)
        def _():
            @pl.when(z > 0)
            def _():
                reduce(c, z + dist, 1, False).wait_recv()
                add_into(c, z + dist)

            reduce(c, z + dist, 1, False).start()

        @pl.when(z >= dist)
        def _():
            @pl.when(z < last)
            def _():
                reduce(c, z - dist, -1, False).wait_recv()
                add_into(c, z - dist)

            reduce(c, z - dist, -1, dist == 1).start()

    def reduce_end(c):
        @pl.when(z > 0)
        def _():
            reduce(c, z, 1, False).wait_recv()

        @pl.when(z < last)
        def _():
            reduce(c, z, -1, True).wait_recv()

        @pl.when(z == 0)
        def _():
            work[slot(c, z), :] = (work[slot(c, z), :].astype(f32) + landing2[c].astype(f32)).astype(bf16)

        @pl.when(z == last)
        def _():
            add_into(c, z)

        @pl.when((z > 0) & (z < last))
        def _():
            total = work[slot(c, z), :].astype(f32) + landing[slot(c, z), :].astype(f32) + landing2[c].astype(f32)
            work[slot(c, z), :] = total.astype(bf16)

        for k in (2, 3, 1):
            collect(c, k).start()
        y_in[own_rows(c), :] = work[slot(c, z), :width]

    norm_chunk(0)
    gather_own(0)
    for c in range(1, chunks):
        norm_chunk(c)
    m_swap_done(2)
    for t in range(chunks + 2):
        if 0 < t < chunks:
            gather_own(t)
        if t == 1:
            m_ready(0)
            m_swap_done(3)
            m_ready(1)
        for h in range(1, n_ty):
            if t >= 2:
                reduce_hop(t - 2, h)
            if 1 <= t <= chunks:
                compute(t - 1, h - 1)
            if t < chunks:
                gather_hop(t, h)
            if t == 0 and h == 1:
                m_far_done(4)
            if t == 0 and h == 3:
                m_far_done(5)
        if t >= 2:
            reduce_end(t - 2)

    for c in range(chunks):
        for k in range(1, n_tx):
            collect(c, k).wait_recv()

    def finish(t, carry):
        rows = pl.ds(aligned(t * 128, 128), 128)
        y_ref[rows, :] = (h_v[rows, :].astype(f32) + y_in[rows, :].astype(f32)).astype(bf16)
        return carry

    lax.fori_loop(0, seq_len // 128, finish, 0)

    for c in range(2):
        for k in range(1, n_tx):
            x_copy(c, k).wait_send()
    for k in range(1, n_tx):
        for m in range(3):
            q_copy(k, m, d).wait_send()
            q_copy(k, m, 1 - d).wait_send()
    for src in range(n_ty):
        for k in range(1, n_tx):
            og_copy(src, k).wait_send()
        for g in range(2):
            @pl.when((z >= src) & (z < last))
            def _():
                z_copy(src, g, 1).wait_send()

            @pl.when((z <= src) & (z > 0))
            def _():
                z_copy(src, g, -1).wait_send()

            @pl.when(z != src)
            def _():
                zx_copy(src, g).wait_send()

        @pl.when((z >= src) & (z < last))
        def _():
            p_copy(src, 1).wait_send()

        @pl.when((z <= src) & (z > 0))
        def _():
            p_copy(src, -1).wait_send()

        @pl.when(z != src)
        def _():
            px_copy(src).wait_send()
    for a in range(3):
        m_near(a).wait_send()
        for q in range(2):
            m_far(a, q).wait_send()
            m_swap(a, q).wait_send()
            for h in range(2):
                m_pass(a, q, h).wait_send()
    for c in range(chunks):
        for k in range(1, n_tx):
            spread(c, k).wait_send()
            collect(c, k).wait_send()
        for src in range(n_ty):
            @pl.when((z >= src) & (z < last))
            def _():
                gather(c, src, 1).wait_send()

            @pl.when((z <= src) & (z > 0))
            def _():
                gather(c, src, -1).wait_send()

            @pl.when(z < src)
            def _():
                reduce(c, src, 1, False).wait_send()

            @pl.when(z > src)
            def _():
                reduce(c, src, -1, False).wait_send()


def solution(mesh):
    act_spec = P(("dp", "ty"), None, "tx")
    col_spec = P("tx", "ty")
    row_spec = P("ty", "tx")
    dma = pltpu.SemaphoreType.DMA

    def layer_fn(x_blk, w_q, w_k, w_v, w_o, w_gate, w_up, w_down):
        seq_len, width = x_blk.shape[1:]
        full, ff = N_TX * width, w_gate.shape[1]
        ch = seq_len // N_TX // CHUNKS
        cos_t, sin_t = rotary_tables(seq_len)
        hbm = pl.BlockSpec(memory_space=pl.ANY)
        vmem = pl.BlockSpec(memory_space=pltpu.VMEM)
        out = pl.pallas_call(
            layer_kernel,
            out_shape=jax.ShapeDtypeStruct((seq_len, width), bf16),
            in_specs=[hbm] * 8 + [vmem] * 2,
            out_specs=vmem,
            scratch_shapes=[
                pltpu.VMEM((N_TX, seq_len, width), bf16),
                pltpu.VMEM((N_TY, 2, 2, width, 3 * HEAD_DIM), bf16),
                pltpu.VMEM((N_TY, width, width), bf16),
                pltpu.VMEM((seq_len, 3 * HEAD_DIM), bf16),
                pltpu.VMEM((seq_len, full), bf16),
                pltpu.VMEM((seq_len, width), bf16),
                pltpu.VMEM((full, ff), bf16),
                pltpu.VMEM((full, ff), bf16),
                pltpu.VMEM((ff, full), bf16),
                pltpu.VMEM((CHUNKS, ch, full), bf16),
                pltpu.VMEM((CHUNKS, N_TY, ch, full), bf16),
                pltpu.VMEM((N_TY * ch, ff), bf16),
                pltpu.VMEM((seq_len, full), bf16),
                pltpu.VMEM((seq_len, full), bf16),
                pltpu.VMEM((CHUNKS, ch, full), bf16),
                pltpu.VMEM((seq_len, width), bf16),
                dma((5,)),
                dma((2, 4)), dma((2, 4)),
                dma((4, 3, 2)), dma((4, 3, 2)),
                dma((N_TY, 2, 2)), dma((N_TY, 2)), dma((N_TY, 2)), dma((N_TY, 2)),
                dma((N_TY, 2)), dma((N_TY,)), dma((N_TY,)), dma((N_TY,)),
                dma((N_TY, 4)), dma((N_TY, 4)),
                dma((3,)), dma((3,)), dma((3, 2)), dma((3, 2)), dma((3, 2)), dma((3, 2)), dma((3, 2, 2)), dma((3, 2, 2)),
                dma((CHUNKS, N_TX)), dma((CHUNKS, N_TX)),
                dma((CHUNKS, N_TY, 2)), dma((CHUNKS, N_TY)),
                dma((CHUNKS, N_TY)), dma((CHUNKS, N_TY)), dma((CHUNKS, 1)),
                dma((CHUNKS, N_TX)), dma((CHUNKS, N_TX)),
            ],
            compiler_params=pltpu.CompilerParams(collective_id=1, has_side_effects=True, vmem_limit_bytes=67043328),
            cost_estimate=pl.CostEstimate(flops=8 * seq_len * full * ff, bytes_accessed=6 * full * ff, transcendentals=seq_len * ff),
            name="layer",
        )(x_blk[0], w_q, w_k, w_v, w_o, w_gate, w_up, w_down, cos_t, sin_t)
        return out[None]

    return jax.shard_map(layer_fn, mesh=mesh, in_specs=(act_spec, col_spec, col_spec, col_spec, row_spec, col_spec, col_spec, row_spec), out_specs=act_spec, check_vma=False)
```

```python
import math

import jax
import jax.numpy as jnp
from jax import lax
from jax.experimental import pallas as pl
from jax.experimental.pallas import tpu as pltpu
from jax.sharding import PartitionSpec as P

HEAD_DIM = 128
EPS = 1e-5
THETA = 10000.0
Q_BLOCK = 256
N_TILE = 256
CHUNKS = 4
N_TX = 4
N_TY = 4
N_PIECES = 4

f32, bf16 = jnp.float32, jnp.bfloat16


def layer_norm(values):
    mean_val = jnp.mean(values, axis=-1, keepdims=True)
    var_val = jnp.mean(values * values, axis=-1, keepdims=True) - mean_val * mean_val
    return ((values - mean_val) * lax.rsqrt(var_val + EPS)).astype(bf16)


def layer_kernel(x_ref, wq_ref, wk_ref, wv_ref, wo_ref, wg_ref, wu_ref, wd_ref, y_ref,
                 x_all, w_all, wo_all, qkv_v, o_all, h_v, gate_v, up_v, down_v, h_rows, n_buf, work, landing, landing2, y_in, cos_ref, sin_ref,
                 loc_sem, x_send, x_recv, q_send, q_recv, z_send, z_recv, zx_send, zx_recv, p_send, p_recv, px_send, px_recv,
                 og_send, og_recv, m1_send, m1_recv, my_send, my_recv, mx_send, mx_recv, mf_send, mf_recv,
                 a_send, a_recv, g_send, g_recv, s_send, lo_recv, hi_recv, c_send, c_recv):
    d, z, i = lax.axis_index("dp"), lax.axis_index("ty"), lax.axis_index("tx")
    yy, core = i // 2, i % 2
    n_tx, n_ty, chunks = N_TX, N_TY, CHUNKS
    seq_len, width = x_ref.shape
    full, ff = n_tx * width, gate_v.shape[1]
    quarter = seq_len // n_tx
    ch = quarter // chunks
    half_w = width // 2
    last = n_ty - 1
    MESH = pl.DeviceIdType.MESH

    def tx_to(k):
        return {"tx": i ^ k}

    def remote(src, dst, send, recv, where):
        return pltpu.make_async_remote_copy(src_ref=src, dst_ref=dst, send_sem=send, recv_sem=recv, device_id=where, device_id_type=MESH)

    def aligned(v, m):
        return pl.multiple_of(v, m)

    x_half = seq_len // 2

    def x_copy(c, k):
        rows = pl.ds(c * x_half, x_half)
        if k == 3:
            return remote(x_all.at[i ^ 2, rows], x_all.at[i ^ 2, rows], x_send.at[c, 3], x_recv.at[c, 3], tx_to(1))
        return remote(x_ref.at[rows], x_all.at[i, rows], x_send.at[c, k], x_recv.at[c, k], tx_to(k))

    mats = (wq_ref, wk_ref, wv_ref)

    def q_copy(k, m, h):
        src = mats[m].at[pl.ds(aligned(h * half_w, half_w), half_w), pl.ds(aligned((i ^ k) * HEAD_DIM, HEAD_DIM), HEAD_DIM)]
        dst = w_all.at[z, h, yy, pl.ds(aligned(core * half_w, half_w), half_w), pl.ds(m * HEAD_DIM, HEAD_DIM)]
        if k == 0:
            return pltpu.make_async_copy(src, dst, q_recv.at[0, m, h])
        return remote(src, dst, q_send.at[k, m, h], q_recv.at[k, m, h], tx_to(k))

    def chip_of(g):
        return yy if g == 0 else 1 - yy

    def z_copy(src, g, step):
        block = w_all.at[src, d, chip_of(g)]
        return remote(block, block, z_send.at[src, g, (step + 1) // 2], z_recv.at[src, g], {"ty": z + step})

    def zx_copy(src, g):
        block = w_all.at[src, d, chip_of(g)]
        return remote(block, block, zx_send.at[src, g], zx_recv.at[src, g], {"dp": 1 - d})

    def p_block(src):
        return wo_all.at[src, pl.ds(aligned(d * half_w, half_w), half_w)]

    def p_copy(src, step):
        return remote(p_block(src), p_block(src), p_send.at[src, (step + 1) // 2], p_recv.at[src], {"ty": z + step})

    def px_copy(src):
        return remote(p_block(src), p_block(src), px_send.at[src], px_recv.at[src], {"dp": 1 - d})

    def og_copy(src, k):
        head = (i ^ 2) if k == 3 else i
        block = o_all.at[:, pl.ds(aligned(src * width + head * HEAD_DIM, HEAD_DIM), HEAD_DIM)]
        return remote(block, block, og_send.at[src, k], og_recv.at[src, k], tx_to(1 if k == 3 else k))

    own_w, full_w = (wg_ref, wu_ref, wd_ref), (gate_v, up_v, down_v)
    q_span = ff // 2 // N_PIECES

    def m_span(h, q):
        return pl.ds(aligned((h * N_PIECES + q) * q_span, q_span), q_span)

    def m_slot(a, k, h, q):
        side = pl.ds(k * width, width)
        if a == 2:
            return down_v.at[m_span(h, q), side]
        return full_w[a].at[side, m_span(h, q)]

    def m_part(a, h, q):
        if a == 2:
            return own_w[a].at[m_span(h, q), :]
        return own_w[a].at[:, m_span(h, q)]

    def m_block(a, k):
        if a == 2:
            return down_v.at[:, pl.ds(k * width, width)]
        return full_w[a].at[pl.ds(k * width, width)]

    def m_own(a):
        return pltpu.make_async_copy(own_w[a], m_block(a, 0), loc_sem.at[a])

    def m_near(a):
        return remote(own_w[a], m_block(a, 1), m1_send.at[a], m1_recv.at[a], tx_to(1))

    def m_far(a, q):
        return remote(m_part(a, d, q), m_slot(a, 2, d, q), my_send.at[a, q], my_recv.at[a, q], tx_to(2))

    def m_swap(a, q):
        return remote(m_slot(a, 2, d, q), m_slot(a, 2, d, q), mx_send.at[a, q], mx_recv.at[a, q], {"dp": 1 - d})

    def m_pass(a, q, h):
        return remote(m_slot(a, 2, h, q), m_slot(a, 3, h, q), mf_send.at[a, q, h], mf_recv.at[a, q, h], tx_to(1))

    PIECES = [(a, q) for q in range(N_PIECES) for a in range(2)] + [(2, q) for q in range(N_PIECES)]

    def m_far_start(p):
        m_far(*PIECES[p]).start()

    def m_far_done(p):
        a, q = PIECES[p]
        m_far(a, q).wait_recv()
        m_swap(a, q).start()
        m_pass(a, q, d).start()

    def m_swap_done(p):
        a, q = PIECES[p]
        m_swap(a, q).wait_recv()
        m_pass(a, q, 1 - d).start()

    def m_near_ready(a):
        m_own(a).wait()
        m_near(a).wait_recv()

    def m_ready(a, q):
        for h in range(2):
            m_pass(a, q, h).wait_recv()

    def slot(c, dst):
        return pl.ds(aligned((c * n_ty + dst) * ch, ch), ch)

    def own_rows(c):
        return pl.ds(aligned(i * quarter + c * ch, ch), ch)

    def spread(c, k):
        rows = pl.ds(aligned((i ^ k) * quarter + c * ch, ch), ch)
        return remote(h_v.at[rows], h_rows.at[c, :, pl.ds(k * width, width)], a_send.at[c, k], a_recv.at[c, k], tx_to(k))

    def gather(c, src, step):
        return remote(n_buf.at[c, src], n_buf.at[c, src], g_send.at[c, src, (step + 1) // 2], g_recv.at[c, src], {"ty": z + step})

    half_full = full // 2

    def cols_of(u):
        return pl.ds(u * half_full, half_full)

    def reduce(c, u, dst, step, final):
        src = work.at[slot(c, dst), cols_of(u)]
        if step == 1:
            return remote(src, landing.at[slot(c, dst), cols_of(u)], s_send.at[c, u, dst], lo_recv.at[c, u, dst], {"ty": z + 1})
        if final:
            return remote(src, landing2.at[c, :, cols_of(u)], s_send.at[c, u, dst], hi_recv.at[c, u], {"ty": z - 1})
        return remote(src, landing.at[slot(c, dst), cols_of(u)], s_send.at[c, u, dst], lo_recv.at[c, u, dst], {"ty": z - 1})

    def collect(c, k):
        return remote(work.at[slot(c, z), pl.ds(k * width, width)], y_in.at[own_rows(c)], c_send.at[c, k], c_recv.at[c, k], tx_to(k))

    x_own = pltpu.make_async_copy(x_ref, x_all.at[i], loc_sem.at[3])
    wo_own = pltpu.make_async_copy(wo_ref, wo_all.at[z], loc_sem.at[4])
    for m in range(3):
        for h in range(2):
            q_copy(0, m, h).start()
    x_own.start()
    wo_own.start()

    barrier = pltpu.get_barrier_semaphore()
    for k in range(1, n_tx):
        pl.semaphore_signal(barrier, inc=1, device_id=tx_to(k), device_id_type=MESH)
    pl.semaphore_signal(barrier, inc=1, device_id={"dp": 1 - d}, device_id_type=MESH)

    @pl.when(z > 0)
    def _():
        pl.semaphore_signal(barrier, inc=1, device_id={"ty": z - 1}, device_id_type=MESH)

    @pl.when(z < last)
    def _():
        pl.semaphore_signal(barrier, inc=1, device_id={"ty": z + 1}, device_id_type=MESH)

    @pl.when((z > 0) & (z < last))
    def _():
        pl.semaphore_wait(barrier, n_tx + 2)

    @pl.when((z == 0) | (z == last))
    def _():
        pl.semaphore_wait(barrier, n_tx + 1)

    for m in range(3):
        q_copy(1, m, d).start()
    for k in (2, 3):
        for m in range(3):
            q_copy(k, m, d).start()
    for m in range(3):
        q_copy(1, m, 1 - d).start()
    for c in range(2):
        x_copy(c, 1).start()
    for c in range(2):
        x_copy(c, 2).start()
    for k in (2, 3):
        for m in range(3):
            q_copy(k, m, 1 - d).start()
    m_far_start(0)
    for a in range(3):
        m_own(a).start()

    def both_ways(make):
        @pl.when(z < last)
        def _():
            make(1).start()

        @pl.when(z > 0)
        def _():
            make(-1).start()

    inner = (z > 0) & (z < last)

    def hop(make, swap, h, where):
        if where != "end":
            for src, step in ((z - h, 1), (z + h, -1)):
                @pl.when(inner & (src >= 0) & (src <= last))
                def _():
                    make(src, step).wait_recv()
                    make(src, step).start()
                    if swap is not None:
                        swap(src).start()
        if where != "mid":
            for src, step, edge in ((z - h, 1, last), (z + h, -1, 0)):
                @pl.when(z == edge)
                def _():
                    make(src, step).wait_recv()
                    if swap is not None:
                        swap(src).start()

    def z_hop(g, h, where="both"):
        hop(lambda src, step: z_copy(src, g, step), lambda src: zx_copy(src, g), h, where)

    def p_hop(h, where):
        hop(p_copy, px_copy, h, where)

    def norm_rows(c):
        block = 32

        def body(t, carry):
            rows = pl.ds(aligned(c * x_half + t * block, block), block)
            parts = [x_all[j, rows, :].astype(f32) for j in range(n_tx)]
            normed = layer_norm(jnp.concatenate(parts, axis=1))
            for j in range(n_tx):
                for h in range(2):
                    to = h * (full // 2) + j * half_w
                    work[rows, to:to + half_w] = normed[:, j * width + h * half_w:j * width + (h + 1) * half_w]
            return carry

        lax.fori_loop(0, x_half // block, body, 0)

    def rotary_tables():
        half_dim = HEAD_DIM // 2

        def body(t, carry):
            rows = pl.ds(aligned(t * 128, 128), 128)
            pos = (t * 128 + lax.broadcasted_iota(jnp.int32, (128, HEAD_DIM), 0)).astype(f32)
            lane = lax.broadcasted_iota(jnp.int32, (128, HEAD_DIM), 1)
            pair = (lane % half_dim).astype(f32)
            angles = pos * jnp.exp(pair * (-2.0 / HEAD_DIM * math.log(THETA)))
            sin_t = jnp.sin(angles)
            cos_ref[rows, :] = jnp.cos(angles)
            sin_ref[rows, :] = jnp.where(lane < half_dim, -sin_t, sin_t)
            return carry

        lax.fori_loop(0, seq_len // 128, body, 0)

    order = [z, (z - 1) * (z - 1) - 2 * (z // 3), 2 + z // 2 - 2 * (z // 3), 3 - 3 * (z // 2)]

    def project_heads(src):
        tile = 256

        def body(t, carry):
            rows = pl.ds(aligned(t * tile, tile), tile)
            weight = w_all[src].reshape(full, 3 * HEAD_DIM)
            qkv_v[rows, :] = jnp.dot(work[rows, :], weight, preferred_element_type=f32).astype(bf16)
            return carry

        lax.fori_loop(0, seq_len // tile, body, 0)

    def rotate(values_bf, rows):
        values = values_bf.astype(f32)
        turned = values * cos_ref[rows, :] + pltpu.roll(values, HEAD_DIM // 2, 1) * sin_ref[rows, :]
        return turned.astype(bf16)

    def attend(src):
        cols = pl.ds(aligned(src * width + i * HEAD_DIM, HEAD_DIM), HEAD_DIM)
        k_rot = rotate(qkv_v[:, HEAD_DIM:2 * HEAD_DIM], slice(0, seq_len))
        v_all = qkv_v[:, 2 * HEAD_DIM:3 * HEAD_DIM]
        for blk in range(seq_len // Q_BLOCK):
            rows = slice(blk * Q_BLOCK, (blk + 1) * Q_BLOCK)
            keys = (blk + 1) * Q_BLOCK
            q_rot = rotate(qkv_v[rows, :HEAD_DIM], rows)
            scores = lax.dot_general(q_rot, k_rot[:keys], (((1,), (1,)), ((), ())), preferred_element_type=f32) * HEAD_DIM ** -0.5
            q_pos = blk * Q_BLOCK + lax.broadcasted_iota(jnp.int32, (Q_BLOCK, keys), 0)
            k_pos = lax.broadcasted_iota(jnp.int32, (Q_BLOCK, keys), 1)
            scores = jnp.where(q_pos >= k_pos, scores, -1e30)
            weights = jnp.exp(scores - jnp.max(scores, axis=-1, keepdims=True))
            probs = (weights * (1.0 / jnp.sum(weights, axis=-1, keepdims=True))).astype(bf16)
            o_all[rows, cols] = jnp.dot(probs, v_all[:keys], preferred_element_type=f32).astype(bf16)

    def og_start(r):
        og_copy(order[r], 2).start()
        og_copy(order[r], 1).start()

    def og_pass(r):
        og_copy(order[r], 2).wait_recv()
        og_copy(order[r], 3).start()

    def block_ready(r):
        for g in range(2):
            zx_copy(order[r], g).wait_recv()

    for m in range(3):
        for h in range(2):
            q_copy(0, m, h).wait()
        q_copy(1, m, d).wait_recv()
    both_ways(lambda step: z_copy(z, 0, step))
    rotary_tables()
    for k in (2, 3):
        for m in range(3):
            q_copy(k, m, d).wait_recv()
    both_ways(lambda step: z_copy(z, 1, step))
    wo_own.wait()
    z_hop(0, 1)
    x_own.wait()
    for c in range(2):
        x_copy(c, 1).wait_recv()
    x_copy(0, 2).wait_recv()
    x_copy(0, 3).start()
    z_hop(1, 1)
    x_copy(0, 3).wait_recv()
    norm_rows(0)
    z_hop(0, 2)
    x_copy(1, 2).wait_recv()
    x_copy(1, 3).start()
    z_hop(1, 2)
    both_ways(lambda step: p_copy(z, step))
    x_copy(1, 3).wait_recv()
    norm_rows(1)
    m_near(0).start()
    for m in range(3):
        q_copy(1, m, 1 - d).wait_recv()
    block_ready(1)
    project_heads(order[1])
    attend(order[1])
    og_start(1)
    m_far_start(1)
    z_hop(0, 3)
    for k in (2, 3):
        for m in range(3):
            q_copy(k, m, 1 - d).wait_recv()
    project_heads(order[0])
    p_hop(1, "mid")
    attend(order[0])
    og_start(0)
    m_near(1).start()
    m_far_start(2)
    z_hop(1, 3)
    block_ready(2)
    project_heads(order[2])
    attend(order[2])
    og_start(2)
    m_near(2).start()
    p_hop(2, "mid")
    og_pass(1)
    og_pass(0)
    p_hop(1, "end")
    block_ready(3)
    project_heads(order[3])
    attend(order[3])
    og_start(3)
    m_far_start(3)
    m_far_start(4)
    p_hop(2, "end")
    og_pass(2)
    p_hop(3, "end")
    m_far_done(0)
    m_far_done(1)
    og_pass(3)
    m_far_done(2)
    for r in range(1, n_ty):
        px_copy(order[r]).wait_recv()
    for r in range(n_ty):
        og_copy(order[r], 1).wait_recv()
        og_copy(order[r], 3).wait_recv()

    def out_project(t, carry):
        rows = pl.ds(aligned(t * 256, 256), 256)
        attn_out = jnp.dot(o_all[rows, :], wo_all[...].reshape(full, width), preferred_element_type=f32).astype(bf16)
        h_v[rows, :] = (x_all[i, rows, :].astype(f32) + attn_out.astype(f32)).astype(bf16)
        return carry

    lax.fori_loop(0, seq_len // 256, out_project, 0)

    for c in range(chunks):
        for k in (2, 3, 1):
            spread(c, k).start()
    for p in range(5, 12):
        m_far_start(p)
    for src in range(n_ty):
        for k in range(1, n_tx):
            og_copy(src, k).wait_send()
    m_far_done(3)

    def norm_chunk(c):
        for k in range(1, n_tx):
            spread(c, k).wait_recv()
        h_rows[c, :, :width] = h_v[own_rows(c), :]
        block = min(ch, 32)
        for b in range(ch // block):
            rows = slice(b * block, (b + 1) * block)
            n_buf[c, z, rows, :] = layer_norm(h_rows[c, rows, :].astype(f32))

    def gather_own(c):
        both_ways(lambda step: gather(c, z, step))

    def gather_hop(c, h):
        hop(lambda src, step: gather(c, src, step), None, h, "mid")

    def gather_ends(c):
        for h in range(1, n_ty):
            hop(lambda src, step: gather(c, src, step), None, h, "end")

    n_tiles, d_tiles = ff // N_TILE, full // N_TILE

    def chunk_rows(c):
        return pl.ds(c * n_ty * ch, n_ty * ch)

    def gate_up(c, lo, hi):
        def body(t, carry):
            cols = pl.ds(aligned(t * N_TILE, N_TILE), N_TILE)
            rows = n_buf[c].reshape(n_ty * ch, full)
            gate_val = jnp.dot(rows, gate_v[:, cols], preferred_element_type=f32).astype(bf16).astype(f32)
            up_val = jnp.dot(rows, up_v[:, cols], preferred_element_type=f32).astype(bf16).astype(f32)
            o_all[chunk_rows(c), cols] = (gate_val * jax.nn.sigmoid(gate_val) * up_val).astype(bf16)
            return carry

        lax.fori_loop(lo, hi, body, 0)

    def first_gate_up(q):
        m_ready(0, q)
        m_ready(1, q)
        gate_up(0, q, q + 1)
        gate_up(0, N_PIECES + q, N_PIECES + q + 1)

    def down(c, u):
        def body(t, carry):
            cols = pl.ds(aligned(t * N_TILE, N_TILE), N_TILE)
            work[chunk_rows(c), cols] = jnp.dot(o_all[chunk_rows(c), :], down_v[:, cols], preferred_element_type=f32).astype(bf16)
            return carry

        lax.fori_loop(u * d_tiles // 2, (u + 1) * d_tiles // 2, body, 0)

    def add_into(c, u, dst):
        rows, cols = slot(c, dst), cols_of(u)
        work[rows, cols] = (work[rows, cols].astype(f32) + landing[rows, cols].astype(f32)).astype(bf16)

    def reduce_hop(c, u, h):
        dist = n_ty - h

        @pl.when(z + dist <= last)
        def _():
            @pl.when(z > 0)
            def _():
                reduce(c, u, z + dist, 1, False).wait_recv()
                add_into(c, u, z + dist)

            reduce(c, u, z + dist, 1, False).start()

        @pl.when(z >= dist)
        def _():
            @pl.when(z < last)
            def _():
                reduce(c, u, z - dist, -1, False).wait_recv()
                add_into(c, u, z - dist)

            reduce(c, u, z - dist, -1, dist == 1).start()

    def reduce_end(c, u):
        rows, cols = slot(c, z), cols_of(u)

        @pl.when(z > 0)
        def _():
            reduce(c, u, z, 1, False).wait_recv()

        @pl.when(z < last)
        def _():
            reduce(c, u, z, -1, True).wait_recv()

        @pl.when(z == 0)
        def _():
            work[rows, cols] = (work[rows, cols].astype(f32) + landing2[c, :, cols].astype(f32)).astype(bf16)

        @pl.when(z == last)
        def _():
            add_into(c, u, z)

        @pl.when((z > 0) & (z < last))
        def _():
            total = work[rows, cols].astype(f32) + landing[rows, cols].astype(f32) + landing2[c, :, cols].astype(f32)
            work[rows, cols] = total.astype(bf16)

        if u == 0:
            collect(c, 1).start()
            y_in[own_rows(c), :] = work[rows, :width]
        else:
            collect(c, 2).start()
            collect(c, 3).start()

    mid = n_tiles // 2
    norm_chunk(0)
    gather_own(0)
    m_far_done(4)
    norm_chunk(1)
    m_swap_done(0)
    norm_chunk(2)
    m_swap_done(1)
    norm_chunk(3)
    m_swap_done(2)
    gather_hop(0, 1)
    gather_own(1)
    m_swap_done(3)
    for a in range(3):
        m_near_ready(a)
    gather_hop(0, 2)
    m_far_done(5)
    m_swap_done(4)
    gather_hop(1, 1)
    gather_own(2)
    m_far_done(6)
    m_swap_done(5)
    m_far_done(7)
    gather_hop(1, 2)
    gather_ends(0)
    first_gate_up(0)
    first_gate_up(1)
    m_swap_done(6)
    gather_hop(2, 1)
    gather_own(3)
    first_gate_up(2)
    m_swap_done(7)
    m_far_done(8)
    first_gate_up(3)
    down(0, 0)
    reduce_hop(0, 0, 1)
    gather_hop(2, 2)
    m_far_done(9)
    gather_ends(1)
    gate_up(1, 0, mid)
    reduce_hop(0, 0, 2)
    m_swap_done(8)
    m_far_done(10)
    gather_hop(3, 1)
    gate_up(1, mid, n_tiles)
    down(1, 0)
    reduce_hop(1, 0, 1)
    reduce_hop(0, 0, 3)
    m_swap_done(9)
    m_far_done(11)
    gather_hop(3, 2)
    gather_ends(2)
    gate_up(2, 0, mid)
    reduce_hop(1, 0, 2)
    m_swap_done(10)
    reduce_end(0, 0)
    gate_up(2, mid, n_tiles)
    reduce_hop(1, 0, 3)
    m_swap_done(11)
    for q in range(N_PIECES):
        m_ready(2, q)
    down(0, 1)
    reduce_hop(0, 1, 1)
    down(2, 0)
    reduce_hop(2, 0, 1)
    down(1, 1)
    reduce_hop(1, 1, 1)
    reduce_hop(0, 1, 2)
    down(2, 1)
    reduce_hop(2, 1, 1)
    reduce_hop(2, 0, 2)
    reduce_end(1, 0)
    gather_ends(3)
    gate_up(3, 0, mid)
    reduce_hop(0, 1, 3)
    reduce_hop(1, 1, 2)
    reduce_hop(2, 1, 2)
    gate_up(3, mid, n_tiles)
    reduce_hop(2, 0, 3)
    reduce_hop(1, 1, 3)
    down(3, 0)
    reduce_hop(3, 0, 1)
    reduce_end(0, 1)
    down(3, 1)
    reduce_hop(3, 1, 1)
    reduce_hop(2, 1, 3)
    reduce_end(2, 0)
    reduce_hop(3, 0, 2)
    reduce_end(1, 1)
    reduce_hop(3, 1, 2)
    reduce_end(2, 1)
    reduce_hop(3, 0, 3)
    reduce_hop(3, 1, 3)
    reduce_end(3, 0)
    reduce_end(3, 1)

    for c in range(chunks):
        for k in range(1, n_tx):
            collect(c, k).wait_recv()

    def finish(t, carry):
        rows = pl.ds(aligned(t * 128, 128), 128)
        y_ref[rows, :] = (h_v[rows, :].astype(f32) + y_in[rows, :].astype(f32)).astype(bf16)
        return carry

    lax.fori_loop(0, seq_len // 128, finish, 0)

    for c in range(2):
        for k in range(1, n_tx):
            x_copy(c, k).wait_send()
    for k in range(1, n_tx):
        for m in range(3):
            q_copy(k, m, d).wait_send()
            q_copy(k, m, 1 - d).wait_send()
    for src in range(n_ty):
        for g in range(2):
            @pl.when((z >= src) & (z < last))
            def _():
                z_copy(src, g, 1).wait_send()

            @pl.when((z <= src) & (z > 0))
            def _():
                z_copy(src, g, -1).wait_send()

            @pl.when(z != src)
            def _():
                zx_copy(src, g).wait_send()

        @pl.when(z != src)
        def _():
            px_copy(src).wait_send()

        @pl.when((z >= src) & (z < last))
        def _():
            p_copy(src, 1).wait_send()

        @pl.when((z <= src) & (z > 0))
        def _():
            p_copy(src, -1).wait_send()

    for a in range(3):
        m_near(a).wait_send()
        for q in range(N_PIECES):
            m_far(a, q).wait_send()
            m_swap(a, q).wait_send()
            for h in range(2):
                m_pass(a, q, h).wait_send()
    for c in range(chunks):
        for k in range(1, n_tx):
            spread(c, k).wait_send()
            collect(c, k).wait_send()
        for src in range(n_ty):
            @pl.when((z >= src) & (z < last))
            def _():
                gather(c, src, 1).wait_send()

            @pl.when((z <= src) & (z > 0))
            def _():
                gather(c, src, -1).wait_send()

            for u in range(2):
                @pl.when(z < src)
                def _():
                    reduce(c, u, src, 1, False).wait_send()

                @pl.when(z > src)
                def _():
                    reduce(c, u, src, -1, False).wait_send()


def solution(mesh):
    act_spec = P(("dp", "ty"), None, "tx")
    col_spec = P("tx", "ty")
    row_spec = P("ty", "tx")
    dma = pltpu.SemaphoreType.DMA

    def layer_fn(x_blk, w_q, w_k, w_v, w_o, w_gate, w_up, w_down):
        seq_len, width = x_blk.shape[1:]
        full, ff = N_TX * width, w_gate.shape[1]
        ch = seq_len // N_TX // CHUNKS
        hbm = pl.BlockSpec(memory_space=pl.ANY)
        vmem = pl.BlockSpec(memory_space=pltpu.VMEM)
        out = pl.pallas_call(
            layer_kernel,
            out_shape=jax.ShapeDtypeStruct((seq_len, width), bf16),
            in_specs=[hbm] * 8,
            out_specs=vmem,
            scratch_shapes=[
                pltpu.VMEM((N_TX, seq_len, width), bf16),
                pltpu.VMEM((N_TY, 2, 2, width, 3 * HEAD_DIM), bf16),
                pltpu.VMEM((N_TY, width, width), bf16),
                pltpu.VMEM((seq_len, 3 * HEAD_DIM), bf16),
                pltpu.VMEM((seq_len, full), bf16),
                pltpu.VMEM((seq_len, width), bf16),
                pltpu.VMEM((full, ff), bf16),
                pltpu.VMEM((full, ff), bf16),
                pltpu.VMEM((ff, full), bf16),
                pltpu.VMEM((CHUNKS, ch, full), bf16),
                pltpu.VMEM((CHUNKS, N_TY, ch, full), bf16),
                pltpu.VMEM((seq_len, full), bf16),
                pltpu.VMEM((seq_len, full), bf16),
                pltpu.VMEM((CHUNKS, ch, full), bf16),
                pltpu.VMEM((seq_len, width), bf16),
                pltpu.VMEM((seq_len, HEAD_DIM), f32),
                pltpu.VMEM((seq_len, HEAD_DIM), f32),
                dma((5,)),
                dma((2, 4)), dma((2, 4)),
                dma((4, 3, 2)), dma((4, 3, 2)),
                dma((N_TY, 2, 2)), dma((N_TY, 2)), dma((N_TY, 2)), dma((N_TY, 2)),
                dma((N_TY, 2)), dma((N_TY,)), dma((N_TY,)), dma((N_TY,)),
                dma((N_TY, 4)), dma((N_TY, 4)),
                dma((3,)), dma((3,)),
                dma((3, N_PIECES)), dma((3, N_PIECES)), dma((3, N_PIECES)), dma((3, N_PIECES)), dma((3, N_PIECES, 2)), dma((3, N_PIECES, 2)),
                dma((CHUNKS, N_TX)), dma((CHUNKS, N_TX)),
                dma((CHUNKS, N_TY, 2)), dma((CHUNKS, N_TY)),
                dma((CHUNKS, 2, N_TY)), dma((CHUNKS, 2, N_TY)), dma((CHUNKS, 2)),
                dma((CHUNKS, N_TX)), dma((CHUNKS, N_TX)),
            ],
            compiler_params=pltpu.CompilerParams(collective_id=1, has_side_effects=True, vmem_limit_bytes=67043328),
            cost_estimate=pl.CostEstimate(flops=8 * seq_len * full * ff, bytes_accessed=6 * full * ff, transcendentals=seq_len * ff),
            name="layer",
        )(x_blk[0], w_q, w_k, w_v, w_o, w_gate, w_up, w_down)
        return out[None]

    return jax.shard_map(layer_fn, mesh=mesh, in_specs=(act_spec, col_spec, col_spec, col_spec, row_spec, col_spec, col_spec, row_spec), out_specs=act_spec, check_vma=False)
```

```python
import math

import jax
import jax.numpy as jnp
from jax import lax
from jax.experimental import pallas as pl
from jax.experimental.pallas import tpu as pltpu
from jax.sharding import PartitionSpec as P

HEAD_DIM = 128
EPS = 1e-5
THETA = 10000.0
Q_BLOCK = 256
N_TILE = 256
CHUNKS = 4
N_TX = 4
N_TY = 4
N_PIECES = 4

f32, bf16 = jnp.float32, jnp.bfloat16


def layer_norm(values):
    mean_val = jnp.mean(values, axis=-1, keepdims=True)
    var_val = jnp.mean(values * values, axis=-1, keepdims=True) - mean_val * mean_val
    return ((values - mean_val) * lax.rsqrt(var_val + EPS)).astype(bf16)


def layer_kernel(x_ref, wq_ref, wk_ref, wv_ref, wo_ref, wg_ref, wu_ref, wd_ref, h_v, y_in,
                 x_all, w_all, wo_all, qkv_v, o_all, gate_v, up_v, down_v, h_rows, n_buf, work, landing, landing2, cos_ref, sin_ref,
                 loc_sem, x_send, x_recv, q_send, q_recv, z_send, z_recv, zx_send, zx_recv, p_send, p_recv, px_send, px_recv,
                 og_send, og_recv, m1_send, m1_recv, my_send, my_recv, mx_send, mx_recv, mf_send, mf_recv,
                 a_send, a_recv, g_send, g_recv, s_send, lo_recv, hi_recv, c_send, c_recv):
    d, z, i = lax.axis_index("dp"), lax.axis_index("ty"), lax.axis_index("tx")
    yy, core = i // 2, i % 2
    n_tx, n_ty, chunks = N_TX, N_TY, CHUNKS
    seq_len, width = x_ref.shape
    full, ff = n_tx * width, gate_v.shape[1]
    quarter = seq_len // n_tx
    ch = quarter // chunks
    half_w = width // 2
    last = n_ty - 1
    MESH = pl.DeviceIdType.MESH

    def tx_to(k):
        return {"tx": i ^ k}

    def remote(src, dst, send, recv, where):
        return pltpu.make_async_remote_copy(src_ref=src, dst_ref=dst, send_sem=send, recv_sem=recv, device_id=where, device_id_type=MESH)

    def aligned(v, m):
        return pl.multiple_of(v, m)

    x_half = seq_len // 2

    def x_copy(c, k):
        rows = pl.ds(c * x_half, x_half)
        if k == 3:
            return remote(x_all.at[i ^ 2, rows], x_all.at[i ^ 2, rows], x_send.at[c, 3], x_recv.at[c, 3], tx_to(1))
        return remote(x_ref.at[rows], x_all.at[i, rows], x_send.at[c, k], x_recv.at[c, k], tx_to(k))

    mats = (wq_ref, wk_ref, wv_ref)

    def q_copy(k, m, h):
        src = mats[m].at[pl.ds(aligned(h * half_w, half_w), half_w), pl.ds(aligned((i ^ k) * HEAD_DIM, HEAD_DIM), HEAD_DIM)]
        dst = w_all.at[z, h, yy, pl.ds(aligned(core * half_w, half_w), half_w), pl.ds(m * HEAD_DIM, HEAD_DIM)]
        if k == 0:
            return pltpu.make_async_copy(src, dst, q_recv.at[0, m, h])
        return remote(src, dst, q_send.at[k, m, h], q_recv.at[k, m, h], tx_to(k))

    def z_block(src, g):
        chip = yy if g < 2 else 1 - yy
        part = core if g % 2 == 0 else 1 - core
        return w_all.at[src, d, chip, pl.ds(aligned(part * half_w, half_w), half_w)]

    def z_copy(src, g, step):
        return remote(z_block(src, g), z_block(src, g), z_send.at[src, g, (step + 1) // 2], z_recv.at[src, g], {"ty": z + step})

    def zx_copy(src, g):
        return remote(z_block(src, g), z_block(src, g), zx_send.at[src, g], zx_recv.at[src, g], {"dp": 1 - d})

    def p_block(src):
        return wo_all.at[src, pl.ds(aligned(d * half_w, half_w), half_w)]

    def p_copy(src, step):
        return remote(p_block(src), p_block(src), p_send.at[src, (step + 1) // 2], p_recv.at[src], {"ty": z + step})

    def p_whole(src, step):
        return remote(wo_all.at[src], wo_all.at[src], p_send.at[src, (step + 1) // 2], p_recv.at[src], {"ty": z + step})

    def px_copy(src):
        return remote(p_block(src), p_block(src), px_send.at[src], px_recv.at[src], {"dp": 1 - d})

    def og_copy(src, k, t):
        head = (i ^ 2) if k == 3 else i
        block = o_all.at[pl.ds(t * x_half, x_half), pl.ds(aligned(src * width + head * HEAD_DIM, HEAD_DIM), HEAD_DIM)]
        return remote(block, block, og_send.at[src, k, t], og_recv.at[src, k, t], tx_to(1 if k == 3 else k))

    own_w, full_w = (wg_ref, wu_ref, wd_ref), (gate_v, up_v, down_v)
    q_span = ff // 2 // N_PIECES

    def m_span(h, q):
        return pl.ds(aligned((h * N_PIECES + q) * q_span, q_span), q_span)

    def m_slot(a, k, h, q):
        side = pl.ds(k * width, width)
        if a == 2:
            return down_v.at[m_span(h, q), side]
        return full_w[a].at[side, m_span(h, q)]

    def m_part(a, h, q):
        if a == 2:
            return own_w[a].at[m_span(h, q), :]
        return own_w[a].at[:, m_span(h, q)]

    def m_block(a, k):
        if a == 2:
            return down_v.at[:, pl.ds(k * width, width)]
        return full_w[a].at[pl.ds(k * width, width)]

    def m_own(a):
        return pltpu.make_async_copy(own_w[a], m_block(a, 0), loc_sem.at[a])

    def m_near(a):
        return remote(own_w[a], m_block(a, 1), m1_send.at[a], m1_recv.at[a], tx_to(1))

    def m_far(a, q):
        return remote(m_part(a, d, q), m_slot(a, 2, d, q), my_send.at[a, q], my_recv.at[a, q], tx_to(2))

    def m_swap(a, q):
        return remote(m_slot(a, 2, d, q), m_slot(a, 2, d, q), mx_send.at[a, q], mx_recv.at[a, q], {"dp": 1 - d})

    def m_pass(a, q, h):
        return remote(m_slot(a, 2, h, q), m_slot(a, 3, h, q), mf_send.at[a, q, h], mf_recv.at[a, q, h], tx_to(1))

    PIECES = [(a, q) for q in range(N_PIECES) for a in range(2)] + [(2, q) for q in range(N_PIECES)]

    def m_far_start(p):
        m_far(*PIECES[p]).start()

    def m_far_done(p):
        a, q = PIECES[p]
        m_far(a, q).wait_recv()
        m_swap(a, q).start()
        m_pass(a, q, d).start()

    def m_swap_done(p):
        a, q = PIECES[p]
        m_swap(a, q).wait_recv()
        m_pass(a, q, 1 - d).start()

    def m_near_ready(a):
        m_own(a).wait()
        m_near(a).wait_recv()

    def m_ready(a, q):
        for h in range(2):
            m_pass(a, q, h).wait_recv()

    def slot(c, dst):
        return pl.ds(aligned((c * n_ty + dst) * ch, ch), ch)

    def own_rows(c):
        return pl.ds(aligned(i * quarter + c * ch, ch), ch)

    def spread(c, k):
        rows = pl.ds(aligned((i ^ k) * quarter + c * ch, ch), ch)
        return remote(h_v.at[rows], h_rows.at[c, :, pl.ds(k * width, width)], a_send.at[c, k], a_recv.at[c, k], tx_to(k))

    def gather(c, src, step):
        return remote(n_buf.at[c, src], n_buf.at[c, src], g_send.at[c, src, (step + 1) // 2], g_recv.at[c, src], {"ty": z + step})

    half_full = full // 2

    def cols_of(u):
        return pl.ds(u * half_full, half_full)

    def reduce(c, u, dst, step, final):
        src = work.at[slot(c, dst), cols_of(u)]
        if step == 1:
            return remote(src, landing.at[slot(c, dst), cols_of(u)], s_send.at[c, u, dst], lo_recv.at[c, u, dst], {"ty": z + 1})
        if final:
            return remote(src, landing2.at[c, :, cols_of(u)], s_send.at[c, u, dst], hi_recv.at[c, u], {"ty": z - 1})
        return remote(src, landing.at[slot(c, dst), cols_of(u)], s_send.at[c, u, dst], lo_recv.at[c, u, dst], {"ty": z - 1})

    def collect(c, k):
        return remote(work.at[slot(c, z), pl.ds(k * width, width)], y_in.at[own_rows(c)], c_send.at[c, k], c_recv.at[c, k], tx_to(k))

    x_own = pltpu.make_async_copy(x_ref, x_all.at[i], loc_sem.at[3])
    wo_own = pltpu.make_async_copy(wo_ref, wo_all.at[z], loc_sem.at[4])
    for m in range(3):
        for h in range(2):
            q_copy(0, m, h).start()
    x_own.start()
    wo_own.start()

    barrier = pltpu.get_barrier_semaphore()
    for k in range(1, n_tx):
        pl.semaphore_signal(barrier, inc=1, device_id=tx_to(k), device_id_type=MESH)
    pl.semaphore_signal(barrier, inc=1, device_id={"dp": 1 - d}, device_id_type=MESH)

    @pl.when(z > 0)
    def _():
        pl.semaphore_signal(barrier, inc=1, device_id={"ty": z - 1}, device_id_type=MESH)

    @pl.when(z < last)
    def _():
        pl.semaphore_signal(barrier, inc=1, device_id={"ty": z + 1}, device_id_type=MESH)

    @pl.when((z > 0) & (z < last))
    def _():
        pl.semaphore_wait(barrier, n_tx + 2)

    @pl.when((z == 0) | (z == last))
    def _():
        pl.semaphore_wait(barrier, n_tx + 1)

    for m in range(3):
        q_copy(1, m, d).start()
    for k in (2, 3):
        for m in range(3):
            q_copy(k, m, d).start()
    for m in range(3):
        q_copy(1, m, 1 - d).start()
    for c in range(2):
        x_copy(c, 1).start()
    for c in range(2):
        x_copy(c, 2).start()
    for m in range(3):
        q_copy(2, m, 1 - d).start()
    m_far_start(0)
    for a in range(3):
        m_own(a).start()

    def both_ways(make):
        @pl.when(z < last)
        def _():
            make(1).start()

        @pl.when(z > 0)
        def _():
            make(-1).start()

    inner = (z > 0) & (z < last)

    def hop(make, swap, h, where):
        if where != "end":
            for src, step in ((z - h, 1), (z + h, -1)):
                @pl.when(inner & (src >= 0) & (src <= last))
                def _():
                    make(src, step).wait_recv()
                    make(src, step).start()
                    if swap is not None:
                        swap(src).start()
        if where != "mid":
            for src, step, edge in ((z - h, 1, last), (z + h, -1, 0)):
                @pl.when(z == edge)
                def _():
                    make(src, step).wait_recv()
                    if swap is not None:
                        swap(src).start()

    def z_hop(g, h, where="both"):
        hop(lambda src, step: z_copy(src, g, step), lambda src: zx_copy(src, g), h, where)

    def at_edge(src):
        return (src == 0) | (src == last)

    def p_step(src, step, onward):
        @pl.when(at_edge(src))
        def _():
            p_whole(src, step).wait_recv()
            if onward:
                p_whole(src, step).start()

        @pl.when(jnp.logical_not(at_edge(src)))
        def _():
            p_copy(src, step).wait_recv()
            if onward:
                p_copy(src, step).start()
            px_copy(src).start()

    def p_hop(h, where):
        if where == "mid":
            for src, step in ((z - h, 1), (z + h, -1)):
                @pl.when(inner & (src >= 0) & (src <= last))
                def _():
                    p_step(src, step, True)
        else:
            for src, step, edge in ((z - h, 1, last), (z + h, -1, 0)):
                @pl.when(z == edge)
                def _():
                    p_step(src, step, False)

    def p_own():
        @pl.when(z == 0)
        def _():
            p_whole(z, 1).start()

        @pl.when(z == last)
        def _():
            p_whole(z, -1).start()

        @pl.when(inner)
        def _():
            p_copy(z, 1).start()
            p_copy(z, -1).start()

    def norm_rows(c):
        block = 32

        def body(t, carry):
            rows = pl.ds(aligned(c * x_half + t * block, block), block)
            parts = [x_all[j, rows, :].astype(f32) for j in range(n_tx)]
            normed = layer_norm(jnp.concatenate(parts, axis=1))
            for j in range(n_tx):
                for h in range(2):
                    to = h * (full // 2) + j * half_w
                    work[rows, to:to + half_w] = normed[:, j * width + h * half_w:j * width + (h + 1) * half_w]
            return carry

        lax.fori_loop(0, x_half // block, body, 0)

    def rotary_tables():
        half_dim = HEAD_DIM // 2

        def body(t, carry):
            rows = pl.ds(aligned(t * 128, 128), 128)
            pos = (t * 128 + lax.broadcasted_iota(jnp.int32, (128, HEAD_DIM), 0)).astype(f32)
            lane = lax.broadcasted_iota(jnp.int32, (128, HEAD_DIM), 1)
            pair = (lane % half_dim).astype(f32)
            angles = pos * jnp.exp(pair * (-2.0 / HEAD_DIM * math.log(THETA)))
            sin_t = jnp.sin(angles)
            cos_ref[rows, :] = jnp.cos(angles)
            sin_ref[rows, :] = jnp.where(lane < half_dim, -sin_t, sin_t)
            return carry

        lax.fori_loop(0, seq_len // 128, body, 0)

    order = [z, (z - 1) * (z - 1) - 2 * (z // 3), 2 + z // 2 - 2 * (z // 3), 3 - 3 * (z // 2)]

    def project_heads(src):
        tile = 256

        def body(t, carry):
            rows = pl.ds(aligned(t * tile, tile), tile)
            weight = w_all[src].reshape(full, 3 * HEAD_DIM)
            qkv_v[rows, :] = jnp.dot(work[rows, :], weight, preferred_element_type=f32).astype(bf16)
            return carry

        lax.fori_loop(0, seq_len // tile, body, 0)

    def rotate(values_bf, rows):
        values = values_bf.astype(f32)
        turned = values * cos_ref[rows, :] + pltpu.roll(values, HEAD_DIM // 2, 1) * sin_ref[rows, :]
        return turned.astype(bf16)

    def attend(src):
        cols = pl.ds(aligned(src * width + i * HEAD_DIM, HEAD_DIM), HEAD_DIM)
        k_rot = rotate(qkv_v[:, HEAD_DIM:2 * HEAD_DIM], slice(0, seq_len))
        v_all = qkv_v[:, 2 * HEAD_DIM:3 * HEAD_DIM]
        for blk in range(seq_len // Q_BLOCK):
            rows = slice(blk * Q_BLOCK, (blk + 1) * Q_BLOCK)
            keys = (blk + 1) * Q_BLOCK
            q_rot = rotate(qkv_v[rows, :HEAD_DIM], rows)
            scores = lax.dot_general(q_rot, k_rot[:keys], (((1,), (1,)), ((), ())), preferred_element_type=f32) * HEAD_DIM ** -0.5
            q_pos = blk * Q_BLOCK + lax.broadcasted_iota(jnp.int32, (Q_BLOCK, keys), 0)
            k_pos = lax.broadcasted_iota(jnp.int32, (Q_BLOCK, keys), 1)
            scores = jnp.where(q_pos >= k_pos, scores, -1e30)
            weights = jnp.exp(scores - jnp.max(scores, axis=-1, keepdims=True))
            probs = (weights * (1.0 / jnp.sum(weights, axis=-1, keepdims=True))).astype(bf16)
            o_all[rows, cols] = jnp.dot(probs, v_all[:keys], preferred_element_type=f32).astype(bf16)
            if (blk + 1) * Q_BLOCK % x_half == 0:
                t = (blk + 1) * Q_BLOCK // x_half - 1
                og_copy(src, 2, t).start()
                og_copy(src, 1, t).start()

    def og_pass(r, t):
        og_copy(order[r], 2, t).wait_recv()
        og_copy(order[r], 3, t).start()

    def og_ready(r, t):
        og_copy(order[r], 1, t).wait_recv()
        og_copy(order[r], 3, t).wait_recv()

    def block_ready(r):
        for g in range(4):
            zx_copy(order[r], g).wait_recv()

    for m in range(3):
        q_copy(0, m, d).wait()
    both_ways(lambda step: z_copy(z, 0, step))
    for g in (1, 2, 3):
        if g == 2:
            rotary_tables()
            z_hop(0, 1)
        for m in range(3):
            q_copy(g, m, d).wait_recv()
        both_ways(lambda step, g=g: z_copy(z, g, step))
    zx_copy(z, 3).start()
    for m in range(3):
        q_copy(0, m, 1 - d).wait()
    wo_own.wait()
    x_own.wait()
    z_hop(1, 1)
    for c in range(2):
        x_copy(c, 1).wait_recv()
    x_copy(0, 2).wait_recv()
    x_copy(0, 3).start()
    z_hop(2, 1)
    x_copy(0, 3).wait_recv()
    norm_rows(0)
    z_hop(3, 1)
    z_hop(0, 2)
    z_hop(1, 2)
    x_copy(1, 2).wait_recv()
    x_copy(1, 3).start()
    z_hop(2, 2)
    z_hop(3, 2)
    p_own()
    x_copy(1, 3).wait_recv()
    norm_rows(1)
    m_near(0).start()
    for m in range(3):
        q_copy(1, m, 1 - d).wait_recv()
    block_ready(1)
    project_heads(order[1])
    attend(order[1])
    m_far_start(1)
    z_hop(0, 3)
    z_hop(1, 3)
    for m in range(3):
        q_copy(2, m, 1 - d).wait_recv()
    zx_copy(z, 3).wait_recv()
    project_heads(order[0])
    p_hop(1, "mid")
    attend(order[0])
    m_near(1).start()
    z_hop(2, 3)
    z_hop(3, 3)
    block_ready(2)
    project_heads(order[2])
    attend(order[2])
    m_near(2).start()
    p_hop(2, "mid")
    p_hop(1, "end")
    block_ready(3)
    project_heads(order[3])
    attend(order[3])
    m_far_start(2)
    p_hop(2, "end")
    for r in (1, 0, 2):
        for t in range(2):
            og_pass(r, t)
    og_pass(3, 0)
    og_pass(3, 1)
    m_far_done(0)
    m_far_done(1)
    p_hop(3, "end")
    for r in range(3):
        for t in range(2):
            og_ready(r, t)
    for src in range(1, last):
        @pl.when(z != src)
        def _():
            px_copy(src).wait_recv()

    def out_project(t, carry):
        rows = pl.ds(aligned(t * 256, 256), 256)
        attn_out = jnp.dot(o_all[rows, :], wo_all[...].reshape(full, width), preferred_element_type=f32).astype(bf16)
        h_v[rows, :] = (x_all[i, rows, :].astype(f32) + attn_out.astype(f32)).astype(bf16)
        return carry

    og_ready(3, 0)
    lax.fori_loop(0, seq_len // 512, out_project, 0)
    og_ready(3, 1)
    lax.fori_loop(seq_len // 512, seq_len // 256, out_project, 0)

    for c, pieces in ((0, ()), (1, (3,)), (2, (4, 5)), (3, (6, 7, 8, 9, 10, 11))):
        for k in (2, 3, 1):
            spread(c, k).start()
        for p in pieces:
            m_far_start(p)
    for src in range(n_ty):
        for k in range(1, n_tx):
            for t in range(2):
                og_copy(src, k, t).wait_send()

    def norm_chunk(c):
        for k in range(1, n_tx):
            spread(c, k).wait_recv()
        h_rows[c, :, :width] = h_v[own_rows(c), :]
        block = min(ch, 32)
        for b in range(ch // block):
            rows = slice(b * block, (b + 1) * block)
            n_buf[c, z, rows, :] = layer_norm(h_rows[c, rows, :].astype(f32))

    def gather_own(c):
        both_ways(lambda step: gather(c, z, step))

    def gather_hop(c, h):
        hop(lambda src, step: gather(c, src, step), None, h, "mid")

    def gather_ends(c):
        for h in range(1, n_ty):
            hop(lambda src, step: gather(c, src, step), None, h, "end")

    n_tiles, d_tiles = ff // N_TILE, full // N_TILE

    def chunk_rows(c):
        return pl.ds(c * n_ty * ch, n_ty * ch)

    def gate_up(c, lo, hi):
        def body(t, carry):
            cols = pl.ds(aligned(t * N_TILE, N_TILE), N_TILE)
            rows = n_buf[c].reshape(n_ty * ch, full)
            gate_val = jnp.dot(rows, gate_v[:, cols], preferred_element_type=f32).astype(bf16).astype(f32)
            up_val = jnp.dot(rows, up_v[:, cols], preferred_element_type=f32).astype(bf16).astype(f32)
            o_all[chunk_rows(c), cols] = (gate_val * jax.nn.sigmoid(gate_val) * up_val).astype(bf16)
            return carry

        lax.fori_loop(lo, hi, body, 0)

    def first_gate_up(q):
        m_ready(0, q)
        m_ready(1, q)
        gate_up(0, q, q + 1)
        gate_up(0, N_PIECES + q, N_PIECES + q + 1)

    def down(c, u):
        def body(t, carry):
            cols = pl.ds(aligned(t * N_TILE, N_TILE), N_TILE)
            work[chunk_rows(c), cols] = jnp.dot(o_all[chunk_rows(c), :], down_v[:, cols], preferred_element_type=f32).astype(bf16)
            return carry

        lax.fori_loop(u * d_tiles // 2, (u + 1) * d_tiles // 2, body, 0)

    def add_into(c, u, dst):
        rows, cols = slot(c, dst), cols_of(u)
        work[rows, cols] = (work[rows, cols].astype(f32) + landing[rows, cols].astype(f32)).astype(bf16)

    def reduce_hop(c, u, h):
        dist = n_ty - h

        @pl.when(z + dist <= last)
        def _():
            @pl.when(z > 0)
            def _():
                reduce(c, u, z + dist, 1, False).wait_recv()
                add_into(c, u, z + dist)

            reduce(c, u, z + dist, 1, False).start()

        @pl.when(z >= dist)
        def _():
            @pl.when(z < last)
            def _():
                reduce(c, u, z - dist, -1, False).wait_recv()
                add_into(c, u, z - dist)

            reduce(c, u, z - dist, -1, dist == 1).start()

    def reduce_end(c, u):
        rows, cols = slot(c, z), cols_of(u)

        @pl.when(z > 0)
        def _():
            reduce(c, u, z, 1, False).wait_recv()

        @pl.when(z < last)
        def _():
            reduce(c, u, z, -1, True).wait_recv()

        @pl.when(z == 0)
        def _():
            work[rows, cols] = (work[rows, cols].astype(f32) + landing2[c, :, cols].astype(f32)).astype(bf16)

        @pl.when(z == last)
        def _():
            add_into(c, u, z)

        @pl.when((z > 0) & (z < last))
        def _():
            total = work[rows, cols].astype(f32) + landing[rows, cols].astype(f32) + landing2[c, :, cols].astype(f32)
            work[rows, cols] = total.astype(bf16)

        if u == 0:
            collect(c, 1).start()
            y_in[own_rows(c), :] = work[rows, :width]
        else:
            collect(c, 2).start()
            collect(c, 3).start()

    mid = n_tiles // 2
    norm_chunk(0)
    gather_own(0)
    m_swap_done(0)
    m_far_done(2)
    m_swap_done(1)
    norm_chunk(1)
    for a in range(3):
        m_near_ready(a)
    gather_hop(0, 1)
    gather_own(1)
    m_swap_done(2)
    m_far_done(3)
    norm_chunk(2)
    gather_hop(0, 2)
    m_far_done(4)
    gather_hop(1, 1)
    gather_own(2)
    m_swap_done(3)
    m_far_done(5)
    gather_hop(1, 2)
    gather_ends(0)
    first_gate_up(0)
    m_swap_done(4)
    first_gate_up(1)
    norm_chunk(3)
    m_far_done(6)
    gather_hop(2, 1)
    gather_own(3)
    m_swap_done(5)
    first_gate_up(2)
    m_far_done(7)
    m_swap_done(6)
    m_swap_done(7)
    m_far_done(8)
    first_gate_up(3)
    down(0, 0)
    reduce_hop(0, 0, 1)
    m_far_done(9)
    gather_hop(2, 2)
    gather_ends(1)
    gate_up(1, 0, mid)
    gather_hop(3, 1)
    reduce_hop(0, 0, 2)
    gate_up(1, mid, n_tiles)
    m_far_done(10)
    down(1, 0)
    reduce_hop(1, 0, 1)
    reduce_hop(0, 0, 3)
    gather_hop(3, 2)
    m_swap_done(8)
    m_far_done(11)
    reduce_hop(1, 0, 2)
    gather_ends(2)
    gate_up(2, 0, mid)
    m_swap_done(9)
    reduce_hop(1, 0, 3)
    m_swap_done(10)
    gate_up(2, mid, n_tiles)
    down(2, 0)
    reduce_hop(2, 0, 1)
    m_swap_done(11)
    for q in range(N_PIECES):
        m_ready(2, q)
    down(0, 1)
    reduce_hop(0, 1, 1)
    reduce_end(0, 0)
    down(1, 1)
    reduce_hop(1, 1, 1)
    reduce_hop(0, 1, 2)
    reduce_hop(1, 1, 2)
    down(2, 1)
    reduce_hop(2, 1, 1)
    reduce_end(1, 0)
    reduce_hop(0, 1, 3)
    gather_ends(3)
    gate_up(3, 0, mid)
    reduce_hop(1, 1, 3)
    reduce_hop(2, 0, 2)
    reduce_hop(2, 1, 2)
    gate_up(3, mid, n_tiles)
    reduce_hop(2, 0, 3)
    down(3, 1)
    reduce_hop(3, 1, 1)
    reduce_end(0, 1)
    down(3, 0)
    reduce_hop(3, 0, 1)
    reduce_hop(2, 1, 3)
    reduce_end(1, 1)
    reduce_end(2, 0)
    reduce_hop(3, 1, 2)
    reduce_hop(3, 0, 2)
    reduce_end(2, 1)
    reduce_hop(3, 1, 3)
    reduce_hop(3, 0, 3)
    reduce_end(3, 1)
    reduce_end(3, 0)

    for c in range(chunks):
        for k in range(1, n_tx):
            collect(c, k).wait_recv()

    for c in range(2):
        for k in range(1, n_tx):
            x_copy(c, k).wait_send()
    for k in range(1, n_tx):
        for m in range(3):
            q_copy(k, m, d).wait_send()
            if k < 3:
                q_copy(k, m, 1 - d).wait_send()
    for src in range(n_ty):
        for g in range(4):
            @pl.when((z >= src) & (z < last))
            def _():
                z_copy(src, g, 1).wait_send()

            @pl.when((z <= src) & (z > 0))
            def _():
                z_copy(src, g, -1).wait_send()

            if g == 3:
                zx_copy(src, g).wait_send()
            else:
                @pl.when(z != src)
                def _():
                    zx_copy(src, g).wait_send()

        inner_src = 0 < src < last
        if inner_src:
            @pl.when(z != src)
            def _():
                px_copy(src).wait_send()

        p_any = p_copy if inner_src else p_whole

        @pl.when((z >= src) & (z < last))
        def _():
            p_any(src, 1).wait_send()

        @pl.when((z <= src) & (z > 0))
        def _():
            p_any(src, -1).wait_send()

    for a in range(3):
        m_near(a).wait_send()
        for q in range(N_PIECES):
            m_far(a, q).wait_send()
            m_swap(a, q).wait_send()
            for h in range(2):
                m_pass(a, q, h).wait_send()
    for c in range(chunks):
        for k in range(1, n_tx):
            spread(c, k).wait_send()
            collect(c, k).wait_send()
        for src in range(n_ty):
            @pl.when((z >= src) & (z < last))
            def _():
                gather(c, src, 1).wait_send()

            @pl.when((z <= src) & (z > 0))
            def _():
                gather(c, src, -1).wait_send()

            for u in range(2):
                @pl.when(z < src)
                def _():
                    reduce(c, u, src, 1, False).wait_send()

                @pl.when(z > src)
                def _():
                    reduce(c, u, src, -1, False).wait_send()


def solution(mesh):
    act_spec = P(("dp", "ty"), None, "tx")
    col_spec = P("tx", "ty")
    row_spec = P("ty", "tx")
    dma = pltpu.SemaphoreType.DMA

    def layer_fn(x_blk, w_q, w_k, w_v, w_o, w_gate, w_up, w_down):
        seq_len, width = x_blk.shape[1:]
        full, ff = N_TX * width, w_gate.shape[1]
        ch = seq_len // N_TX // CHUNKS
        hbm = pl.BlockSpec(memory_space=pl.ANY)
        vmem = pl.BlockSpec(memory_space=pltpu.VMEM)
        resid_h, mlp_out = pl.pallas_call(
            layer_kernel,
            out_shape=[jax.ShapeDtypeStruct((seq_len, width), bf16)] * 2,
            in_specs=[hbm] * 8,
            out_specs=[vmem] * 2,
            scratch_shapes=[
                pltpu.VMEM((N_TX, seq_len, width), bf16),
                pltpu.VMEM((N_TY, 2, 2, width, 3 * HEAD_DIM), bf16),
                pltpu.VMEM((N_TY, width, width), bf16),
                pltpu.VMEM((seq_len, 3 * HEAD_DIM), bf16),
                pltpu.VMEM((seq_len, full), bf16),
                pltpu.VMEM((full, ff), bf16),
                pltpu.VMEM((full, ff), bf16),
                pltpu.VMEM((ff, full), bf16),
                pltpu.VMEM((CHUNKS, ch, full), bf16),
                pltpu.VMEM((CHUNKS, N_TY, ch, full), bf16),
                pltpu.VMEM((seq_len, full), bf16),
                pltpu.VMEM((seq_len, full), bf16),
                pltpu.VMEM((CHUNKS, ch, full), bf16),
                pltpu.VMEM((seq_len, HEAD_DIM), f32),
                pltpu.VMEM((seq_len, HEAD_DIM), f32),
                dma((5,)),
                dma((2, 4)), dma((2, 4)),
                dma((4, 3, 2)), dma((4, 3, 2)),
                dma((N_TY, 4, 2)), dma((N_TY, 4)), dma((N_TY, 4)), dma((N_TY, 4)),
                dma((N_TY, 2)), dma((N_TY,)), dma((N_TY,)), dma((N_TY,)),
                dma((N_TY, 4, 2)), dma((N_TY, 4, 2)),
                dma((3,)), dma((3,)),
                dma((3, N_PIECES)), dma((3, N_PIECES)), dma((3, N_PIECES)), dma((3, N_PIECES)), dma((3, N_PIECES, 2)), dma((3, N_PIECES, 2)),
                dma((CHUNKS, N_TX)), dma((CHUNKS, N_TX)),
                dma((CHUNKS, N_TY, 2)), dma((CHUNKS, N_TY)),
                dma((CHUNKS, 2, N_TY)), dma((CHUNKS, 2, N_TY)), dma((CHUNKS, 2)),
                dma((CHUNKS, N_TX)), dma((CHUNKS, N_TX)),
            ],
            compiler_params=pltpu.CompilerParams(collective_id=1, has_side_effects=True, vmem_limit_bytes=64487424),
            cost_estimate=pl.CostEstimate(flops=8 * seq_len * full * ff, bytes_accessed=6 * full * ff, transcendentals=seq_len * ff),
            name="layer",
        )(x_blk[0], w_q, w_k, w_v, w_o, w_gate, w_up, w_down)
        return (resid_h.astype(f32) + mlp_out.astype(f32)).astype(bf16)[None]

    return jax.shard_map(layer_fn, mesh=mesh, in_specs=(act_spec, col_spec, col_spec, col_spec, row_spec, col_spec, col_spec, row_spec), out_specs=act_spec, check_vma=False)
```
